32 devices in a mesh: grp: 2 (over y), leaf: 4 (over z), sub: 4 (over x, core).
Axes of the slice: x: 2, y: 2, z: 4, core: 2. Of those that a mesh axis runs over, the one named last changes fastest.
Arguments:
- targets: bfloat16 [64, 65536], P(None, ('grp', 'leaf', 'sub')), parts along dimension 1, may hold values from -6 to 6
- tree_order: int32 [32, 2048], P(('grp', 'leaf', 'sub')), parts along dimension 0, may hold values from 0 to 2047, each once within a row
- leaf_inverse: bfloat16 [128, 512, 512], P(('grp', 'leaf', 'sub')), parts along dimension 0, as said below
- cluster_basis: bfloat16 [6, 32, 65536], P(None, None, ('grp', 'leaf', 'sub')), parts along dimension 2, may hold values from -1.5 to 1.5
- coupling: float32 [32, 6, 32, 64], P(('grp', 'leaf', 'sub')), parts along dimension 0, may hold values from -0.75 to 0.75
- train_coords: bfloat16 [3, 65536], P(None, ('grp', 'leaf', 'sub')), parts along dimension 1, may hold values from 0 to 1
- test_coords: bfloat16 [3, 65536], P(None, ('grp', 'leaf', 'sub')), parts along dimension 1, may hold values from 0 to 1
- test_basis: bfloat16 [4, 32, 65536], P(None, None, ('grp', 'leaf', 'sub')), parts along dimension 2, may hold values from -2.4 to 2.4
- near_leaves: int32 [32, 8], P(('grp', 'leaf', 'sub')), parts along dimension 0, may hold values from 0 to 63, as said below
Outputs:
- posterior_mean: bfloat16 [64, 65536], P(None, ('grp', 'leaf', 'sub')), parts along dimension 1
The draws below stay inside these ranges and needn't reach their ends.
There are 2 independent parts, one for each index of `grp`. The reference program is written for one: setup_inputs(seed, part) draws one part's arguments, and reference() takes and returns one part's arrays. A program takes and returns all parts, laid end to end along the dimension named above; each array names one. Nothing has to cross between parts.
Inputs may be any that keep to these rules, and one draw needn't show every extreme that they name: `tree_order`: row d is a permutation of the positions 0 to 2047 within panel d. `near_leaves`: row d names 8 different training leaves, all held by panels d - 1, d or d + 1. `leaf_inverse`: each block is the identity plus dense full-rank entries of spread 0.5 / sqrt(512).
All inputs are finite; a program needn't handle non-finite values.
Results may differ from the reference program's by a relative error of at most 0.0035.
Values may be sent and summed in bfloat16 or wider, within the bound.
A program may use at most 64 MiB of HBM per device.

```python
import math
import jax
import jax.numpy as jnp
from jax import lax

RHS = 64
LEAF = 512
RANK = 32
NEAR = 8
LEAF_DEV = 4
TEST_DEV = 2048
GROUP_DEVS = 16
PTS_DEV = 2048
NTRAIN = 32768
LEAVES = 64
NTEST = 32768
LOCAL_LEVELS = 2
DEV_LEVELS = 4
LEVELS = 6


def draw_leaf_inverse(key, part):
    noise = jax.random.normal(jax.random.fold_in(key, 11), (LEAVES, LEAF, LEAF), jnp.float32)
    identity = jnp.eye(LEAF, dtype=jnp.float32)[None]
    return (identity + noise * (0.5 / math.sqrt(LEAF))).astype(jnp.bfloat16)


def draw_test_basis(key, part):
    levels = jnp.arange(DEV_LEVELS, dtype=jnp.float32)
    spread = 0.05 * 8.0 ** (levels / (DEV_LEVELS - 1))
    noise = jnp.clip(jax.random.normal(jax.random.fold_in(key, 23), (DEV_LEVELS, RANK, NTEST), jnp.float32), -6.0, 6.0)
    return (noise * spread[:, None, None]).astype(jnp.bfloat16)


def draw_near_leaves(key, part):
    window = 3 * LEAF_DEV
    device_ids = jnp.arange(GROUP_DEVS, dtype=jnp.int32)[:, None]
    candidates = jnp.arange(window, dtype=jnp.int32)[None, :]
    leaf_ids = (device_ids - 1) * LEAF_DEV + candidates
    valid = (leaf_ids >= 0) & (leaf_ids < LEAVES)
    scores = jax.random.randint(jax.random.fold_in(key, 7), (GROUP_DEVS, window), 0, 1 << 20, dtype=jnp.int32) * window + candidates
    scores = jnp.where(valid, scores, -1)
    chosen = lax.top_k(scores, NEAR)[1].astype(jnp.int32)
    return jnp.take_along_axis(leaf_ids, chosen, axis=1).astype(jnp.int32)


def level_of(key, shape, split, low, high):
    factor_of = 1.0
    for position, blocks in split:
        heights = jax.random.uniform(jax.random.fold_in(jax.random.fold_in(key, 6), position), (blocks,), jnp.float32, low / len(split), high / len(split))
        factor_of = factor_of * jnp.repeat(jnp.exp(heights), shape[position] // blocks).reshape((-1,) + (1,) * (len(shape) - 1 - position))
    return factor_of


def scatter_about(rng, extent, deviation, most, cuts=(), kind=jnp.bfloat16):
    entries = jax.random.normal(rng, extent, jnp.float32) * deviation
    if len(cuts) > 0:
        entries = level_of(rng, extent, cuts, -0.22, 0.18) * entries
    return jnp.clip(entries, min=-most, max=most).astype(kind)


def setup_inputs(seed: int = 0, part: int = 0) -> dict:
    key_of = jax.random.split(jax.random.key(seed), 10)
    part_splits = jax.random.split(jax.random.fold_in(key_of[9], part), 10)
    return {
        "targets": scatter_about(part_splits[0], (RHS, NTRAIN), 1.0, 6.0, ((1, 16),)),
        "tree_order": jax.vmap(lambda own: jax.random.permutation(own, PTS_DEV))(jax.random.split(part_splits[1], GROUP_DEVS)).reshape((GROUP_DEVS, PTS_DEV)).astype(jnp.int32),
        "leaf_inverse": draw_leaf_inverse(jax.random.fold_in(jax.random.fold_in(key_of[9], part), 71), part),
        "cluster_basis": scatter_about(part_splits[3], (LEVELS, RANK, NTRAIN), 0.25, 1.5, ((2, 16),)),
        "coupling": scatter_about(part_splits[4], (GROUP_DEVS, LEVELS, RANK, 2 * RANK), (2 * RANK) ** -0.5, 0.75, ((0, 16),), jnp.float32),
        "train_coords": jnp.clip(1.0 * jax.random.uniform(part_splits[5], (3, NTRAIN), jnp.float32) ** level_of(part_splits[5], (3, NTRAIN), ((1, 16),), -0.2, 0.2), 0.0, 1.0).astype(jnp.bfloat16),
        "test_coords": jnp.clip(1.0 * jax.random.uniform(part_splits[6], (3, NTEST), jnp.float32) ** level_of(part_splits[6], (3, NTEST), ((1, 16),), -0.2, 0.2), 0.0, 1.0).astype(jnp.bfloat16),
        "test_basis": draw_test_basis(jax.random.fold_in(jax.random.fold_in(key_of[9], part), 71), part),
        "near_leaves": draw_near_leaves(jax.random.fold_in(jax.random.fold_in(key_of[9], part), 71), part),
    }


variance = 2.0
length_scale = 0.5
highest = lax.Precision.HIGHEST

def matern(train_pos, test_pos):
    train_f32 = train_pos.astype(jnp.float32)
    test_f32 = test_pos.astype(jnp.float32)
    squared = jnp.zeros((train_f32.shape[1], test_f32.shape[1]), jnp.float32)
    for axis_number in range(3):
        offset = train_f32[axis_number][:, None] - test_f32[axis_number][None, :]
        squared = squared + offset * offset
    scaled = jnp.sqrt(3.0 * squared) / length_scale
    return (variance * (1.0 + scaled) * jnp.exp(-scaled)).astype(jnp.bfloat16)

def reference(targets, tree_order, leaf_inverse, cluster_basis, coupling, train_coords, test_coords, test_basis, near_leaves):
    device_base = (jnp.arange(GROUP_DEVS, dtype=jnp.int32) * PTS_DEV)[:, None]
    flat_index = (tree_order + device_base).reshape(-1).astype(jnp.int32)
    reordered = jnp.take(targets, flat_index, axis=1)

    def solve_panel(pair):
        inverse_part, target_part = pair
        return jnp.einsum('jpq,rjq->rjp', inverse_part.astype(jnp.float32), target_part.astype(jnp.float32), precision=highest)
    inverse_groups = leaf_inverse.reshape(GROUP_DEVS, LEAF_DEV, LEAF, LEAF)
    target_groups = reordered.reshape(RHS, GROUP_DEVS, LEAF_DEV, LEAF).transpose(1, 0, 2, 3)
    solved = lax.map(solve_panel, (inverse_groups, target_groups))
    state = solved.transpose(1, 0, 2, 3).reshape(RHS, NTRAIN)
    for level_index in range(LEVELS):
        child = LEAF * 2 ** level_index
        child_count = NTRAIN // child
        unit = min(child, PTS_DEV)
        unit_count = NTRAIN // unit
        level_basis = cluster_basis[level_index].astype(jnp.float32)
        coefficient = jnp.einsum('kcp,rcp->ckr', level_basis.reshape(RANK, child_count, child), state.reshape(RHS, child_count, child), precision=highest) / math.sqrt(child)
        paired = coefficient.reshape(child_count // 2, 2, RANK, RHS)
        sibling = paired[:, ::-1].reshape(child_count, RANK, RHS)
        joined = jnp.concatenate([coefficient, sibling], axis=1)
        per_unit = jnp.repeat(joined, child // unit, axis=0)
        unit_coupling = jnp.repeat(coupling[:, level_index], PTS_DEV // unit, axis=0)
        mixed = jnp.einsum('uks,usr->ukr', unit_coupling, per_unit, precision=highest)
        update = jnp.einsum('ukr,kup->rup', mixed, level_basis.reshape(RANK, unit_count, unit), precision=highest)
        state = (state.reshape(RHS, unit_count, unit) - update).reshape(RHS, NTRAIN)
    weights = state.astype(jnp.bfloat16)
    weight_leaves = weights.reshape(RHS, LEAVES, LEAF)
    coord_leaves = train_coords.reshape(3, LEAVES, LEAF)
    test_groups = test_coords.reshape(3, GROUP_DEVS, TEST_DEV).transpose(1, 0, 2)

    def near_panel(pair):
        leaf_ids, test_pos = pair
        total = jnp.zeros((RHS, TEST_DEV), jnp.float32)
        for slot_index in range(NEAR):
            leaf_id = leaf_ids[slot_index].astype(jnp.int32)
            train_pos = lax.dynamic_index_in_dim(coord_leaves, leaf_id, 1, keepdims=False)
            leaf_weights = lax.dynamic_index_in_dim(weight_leaves, leaf_id, 1, keepdims=False)
            kernel = matern(train_pos, test_pos)
            total = total + jnp.dot(leaf_weights, kernel, preferred_element_type=jnp.float32)
        return total
    near_sum = lax.map(near_panel, (near_leaves, test_groups))
    far = jnp.zeros((RHS, GROUP_DEVS, TEST_DEV), jnp.float32)
    test_levels = test_basis.reshape(DEV_LEVELS, RANK, GROUP_DEVS, TEST_DEV)
    panel_weights = weights.reshape(RHS, GROUP_DEVS, PTS_DEV).astype(jnp.float32)
    for level_index in range(DEV_LEVELS):
        span = 2 ** level_index
        level_basis = cluster_basis[LOCAL_LEVELS + level_index].reshape(RANK, GROUP_DEVS, PTS_DEV).astype(jnp.float32)
        terms = jnp.einsum('kdp,rdp->dkr', level_basis, panel_weights, precision=highest) / math.sqrt(PTS_DEV * span)
        subtree = terms.reshape(GROUP_DEVS // span, span, RANK, RHS).sum(axis=1)
        sibling_ids = (jnp.arange(GROUP_DEVS, dtype=jnp.int32) // span ^ 1).astype(jnp.int32)
        sibling = jnp.take(subtree, sibling_ids, axis=0)
        far = far + jnp.einsum('dkr,kdt->rdt', sibling, test_levels[level_index].astype(jnp.float32), precision=highest)
    mean = near_sum.transpose(1, 0, 2) / math.sqrt(NEAR * LEAF) + far
    return mean.reshape(RHS, NTEST).astype(jnp.bfloat16)
```

```python
import functools
import math

import jax
import jax.numpy as jnp
from jax import lax
from jax.experimental import pallas as pl
from jax.experimental.pallas import tpu as pltpu
from jax.sharding import PartitionSpec as P

variance = 2.0
length_scale = 0.5
f32 = jnp.float32
bf16 = jnp.bfloat16
CHUNK = 256
TILE = 1024
FEATS = 16
EARLY = 7


def nt(a, b):
    return lax.dot_general(a, b, (((1,), (1,)), ((), ())), preferred_element_type=f32)


def nn(a, b):
    return jnp.dot(a, b, preferred_element_type=f32)


def tn(a, b):
    return lax.dot_general(a, b, (((0,), (0,)), ((), ())), preferred_element_type=f32)


def halves(x):
    high = x.astype(bf16)
    return high, (x - high.astype(f32)).astype(bf16)


def thirds(x):
    first = x.astype(bf16).astype(f32)
    second = (x - first).astype(bf16).astype(f32)
    return [first, second, (x - first - second).astype(bf16).astype(f32)]


def toggled(index, mask):
    bit = 1
    while bit <= mask:
        if mask & bit:
            index = index + bit - 2 * bit * lax.rem(lax.div(index, bit), 2)
        bit *= 2
    return index


def triple(a, b):
    ah, al = halves(a)
    bh, bl = halves(b)
    return nn(ah, bh) + nn(ah, bl) + nn(al, bh)


def fold(x):
    rows = x.shape[0] // 4
    return jnp.concatenate([x[q * rows : (q + 1) * rows] for q in range(4)], axis=1)


def unfold(x):
    width = x.shape[1] // 4
    return jnp.concatenate([x[:, q * width : (q + 1) * width] for q in range(4)], axis=0)


def pair(x):
    rows = x.shape[0] // 2
    return jnp.concatenate([x[:rows], x[rows:]], axis=1)


def unpair(x):
    width = x.shape[1] // 2
    return jnp.concatenate([x[:, :width], x[:, width:]], axis=0)


def kernel(
    panels,
    sub_size,
    order_hbm,
    targets_hbm,
    inverse_hbm,
    basis_hbm,
    coupling_hbm,
    train_hbm,
    test_hbm,
    test_basis_hbm,
    near_hbm,
    out_ref,
    order_ref,
    targets_ref,
    inverse_ref,
    basis_ref,
    coupling_ref,
    train_ref,
    test_ref,
    test_basis_ref,
    near_ref,
    cross_sent,
    cross_received,
    sent,
    received,
    far_sent,
    far_received,
    coord_window,
    features,
    test_features,
    blocks,
    weight_window,
    load_sems,
    leaf_sems,
    cross_send,
    cross_recv,
    round_send,
    round_recv,
    far_send,
    far_recv,
    coord_send,
    coord_recv,
    weight_send,
    weight_recv,
):
    columns, points = targets_ref.shape
    leaf_count, leaf_size = inverse_ref.shape[0], inverse_ref.shape[1]
    levels, rank = basis_ref.shape[0], basis_ref.shape[1]
    near = near_ref.shape[1]
    tests = test_ref.shape[1]
    local = leaf_count.bit_length() - 1
    depth = levels - local
    me = lax.axis_index("leaf") * sub_size + lax.axis_index("sub")

    def load(index, source, target):
        copy = pltpu.make_async_copy(source, target, load_sems.at[index])
        copy.start()
        return copy

    basis_copy = load(0, basis_hbm, basis_ref)
    coupling_copy = load(1, coupling_hbm, coupling_ref)
    order_copy = load(2, order_hbm, order_ref)
    targets_copy = load(3, targets_hbm, targets_ref)
    leaf_copies = []
    for leaf in range(leaf_count):
        copy = pltpu.make_async_copy(
            inverse_hbm.at[leaf], inverse_ref.at[leaf], leaf_sems.at[leaf]
        )
        copy.start()
        leaf_copies.append(copy)
    train_copy = load(4, train_hbm, train_ref)
    test_copy = load(5, test_hbm, test_ref)
    near_copy = load(6, near_hbm, near_ref)
    test_basis_copy = load(7, test_basis_hbm, test_basis_ref)

    def device(index):
        return {"leaf": lax.div(index, sub_size), "sub": lax.rem(index, sub_size)}

    barrier = pltpu.get_barrier_semaphore()
    for mask in range(1, panels):
        pl.semaphore_signal(
            barrier,
            inc=1,
            device_id=device(toggled(me, mask)),
            device_id_type=pl.DeviceIdType.MESH,
        )

    def remote(source, target, send, recv, index):
        return pltpu.make_async_remote_copy(
            src_ref=source,
            dst_ref=target,
            send_sem=send,
            recv_sem=recv,
            device_id=device(index),
            device_id_type=pl.DeviceIdType.MESH,
        )

    def shared(copy_next, copy_prev):
        def start():
            pl.when(me < panels - 1)(copy_next.start)
            pl.when(me > 0)(copy_prev.start)

        def wait():
            pl.when(me < panels - 1)(copy_next.wait_send)
            pl.when(me > 0)(copy_prev.wait_send)
            pl.when(me > 0)(copy_next.wait_recv)
            pl.when(me < panels - 1)(copy_prev.wait_recv)

        return start, wait

    after, before = lax.rem(me + 1, panels), lax.rem(me + panels - 1, panels)

    scale = jnp.concatenate(
        [jnp.full((rank, 1), 1.0 / math.sqrt(leaf_size << level), f32) for level in range(levels)],
        axis=0,
    )
    top = local * rank

    def rows_of(level):
        return slice(level * rank, (level + 1) * rank)

    def first_half(x):
        return x[:, :rank]

    def second_half(x):
        return x[:, rank:]

    basis_copy.wait()
    coupling_copy.wait()
    basis = basis_ref[...].reshape(levels * rank, points)
    coupling = [coupling_ref[0, level] for level in range(levels)]
    bases = [basis[:, leaf * leaf_size : (leaf + 1) * leaf_size] for leaf in range(leaf_count)]
    grams = [nt(one, one) for one in bases]

    def transfer(gram, level):
        below = (level + 1) * rank
        return scale[below:] * triple(gram[below:, rows_of(level)], coupling[level])

    gram = sum(one[top:, top:] for one in grams)
    crossing = []
    for k in range(depth - 1):
        below = (k + 1) * rank
        crossing.append(
            scale[top + below :] * triple(gram[below:, rows_of(k)], coupling[local + k])
        )
    cross_rows = [
        sum((depth - 1 - j) * rank for j in range(b, depth - 1)) // 4 for b in range(depth - 1)
    ]
    cross_starts = [sum(cross_rows[:b]) for b in range(depth - 1)]
    slot_starts = [sum((1 << c) * cross_rows[c] for c in range(b)) for b in range(depth - 1)]
    for b in range(depth - 1):
        parts = [second_half(crossing[b])] + [
            first_half(crossing[j]) for j in range(b + 1, depth - 1)
        ]
        cross_sent[pl.ds(cross_starts[b], cross_rows[b])] = fold(jnp.concatenate(parts, axis=0))

    pl.semaphore_wait(barrier, panels - 1)
    train_copy.wait()
    start_coords, wait_coords = shared(
        remote(train_ref, coord_window.at[0], coord_send.at[0], coord_recv.at[0], after),
        remote(train_ref, coord_window.at[1], coord_send.at[1], coord_recv.at[1], before),
    )
    cross_copies = []
    for b in range(depth - 1):
        for mask in range(1 << b, 2 << b):
            place = slot_starts[b] + (mask - (1 << b)) * cross_rows[b]
            copy = remote(
                cross_sent.at[pl.ds(cross_starts[b], cross_rows[b])],
                cross_received.at[pl.ds(place, cross_rows[b])],
                cross_send.at[mask],
                cross_recv.at[mask],
                toggled(me, mask),
            )
            copy.start()
            cross_copies.append(copy)
    start_coords()

    local_sides = []
    for level in range(local):
        width = 1 << level
        parts = [
            transfer(sum(grams[c * width + i] for i in range(width)), level)
            for c in range(leaf_count // width)
        ]
        local_sides.append(
            [first_half(parts[c]) + second_half(parts[c ^ 1]) for c in range(len(parts))]
        )

    order_copy.wait()
    targets_copy.wait()
    stacked = jnp.concatenate(
        [targets_ref[:, h * CHUNK : (h + 1) * CHUNK] for h in range(points // CHUNK)], axis=0
    )
    order = order_ref[...]
    low, high = lax.rem(order, CHUNK), lax.div(order, CHUNK)
    solved, coefs = [], []
    for leaf in range(leaf_count):
        span = slice(leaf * leaf_size, (leaf + 1) * leaf_size)
        places = lax.broadcasted_iota(jnp.int32, (CHUNK, leaf_size), 0)
        chosen = jnp.where(places == low[:, span], 1.0, 0.0).astype(bf16)
        picked = nn(stacked, chosen)
        taken = jnp.zeros((columns, leaf_size), f32)
        for h in range(points // CHUNK):
            taken = jnp.where(
                high[:, span] == h, picked[h * columns : (h + 1) * columns], taken
            )
        leaf_copies[leaf].wait()
        state = nt(taken.astype(bf16), inverse_ref[leaf])
        state_high, state_low = halves(state)
        coefs.append((nt(bases[leaf], state_high) + nt(bases[leaf], state_low)) * scale)
        solved.append(state)

    mixes = [[] for _ in range(leaf_count)]
    for level in range(local):
        sides = local_sides[level]
        heads = [one[:rank] for one in coefs]
        for leaf in range(leaf_count):
            c = leaf >> level
            if leaf == c << level:
                mixed = triple(
                    coupling[level], jnp.concatenate([heads[c], heads[c ^ 1]], axis=0)
                )
            mixes[leaf].append(mixed)
        coefs = [
            coefs[2 * p][rank:]
            + coefs[2 * p + 1][rank:]
            - triple(sides[2 * p], heads[2 * p])
            - triple(sides[2 * p + 1], heads[2 * p + 1])
            for p in range(len(coefs) // 2)
        ]
    own = coefs[0]

    near_copy.wait()
    test_copy.wait()
    gain = 3.0 / (length_scale * length_scale) * math.log2(math.e) ** 2

    def norm(pos):
        return gain * (pos[0:1] * pos[0:1] + pos[1:2] * pos[1:2] + pos[2:3] * pos[2:3])

    def train_side(pos):
        ones = jnp.ones((3, points), f32)
        zero = jnp.zeros((1, points), f32)
        parts = thirds(-2.0 * gain * pos) + thirds(norm(pos)) + [ones, zero]
        return jnp.concatenate(parts, axis=0).astype(bf16)

    def put_features(panel, pos):
        made = train_side(pos.astype(f32))
        for leaf in range(leaf_count):
            features[panel * leaf_count + leaf] = made[:, leaf * leaf_size : (leaf + 1) * leaf_size]

    first_leaf = (me - 1) * leaf_count

    def window_leaf(slot):
        return jnp.clip(near_ref[0, slot] - first_leaf, 0, 3 * leaf_count - 1)

    def near_block(step, carry):
        slot, tile = lax.div(step, tests // TILE), lax.rem(step, tests // TILE)
        lanes = pl.ds(pl.multiple_of(tile * TILE, TILE), TILE)
        squared = tn(features[window_leaf(slot)], test_features[:, lanes])
        squared = jnp.maximum(squared, 1e-12)
        scaled = squared * lax.rsqrt(squared)
        value = (scaled + 1.0 / math.log(2.0)) * jnp.exp2(
            math.log2(variance * math.log(2.0)) - scaled
        )
        blocks[pl.ds(pl.multiple_of(slot * leaf_size, leaf_size), leaf_size), lanes] = value.astype(
            bf16
        )
        return carry

    total_steps = near * (tests // TILE)
    split = total_steps * EARLY // 16

    for copy in cross_copies:
        copy.wait()
    summed = []
    for b in range(depth - 1):
        total = sum(
            cross_received[pl.ds(slot_starts[b] + i * cross_rows[b], cross_rows[b])]
            for i in range(1 << b)
        )
        flat = unfold(total)
        pieces, place = {}, 0
        for j in range(b, depth - 1):
            size = (depth - 1 - j) * rank
            pieces[j] = flat[place : place + size]
            place += size
        summed.append(pieces)
    rest, flows = own, []
    for j in range(depth):
        flows.append(rest[:rank])
        if j < depth - 1:
            side = first_half(crossing[j]) + sum(summed[b][j] for b in range(j + 1))
            rest = rest[rank:] - triple(side, flows[j])
    for k in range(depth):
        sent[k] = pair(flows[k])
    copies = []
    for mask in range(1, panels):
        b = mask.bit_length() - 1
        copy = remote(
            sent.at[pl.ds(b, depth - b)],
            received.at[mask, pl.ds(b, depth - b)],
            round_send.at[mask],
            round_recv.at[mask],
            toggled(me, mask),
        )
        copy.start()
        copies.append(copy)

    test_pos = test_ref[...].astype(f32)
    ones = jnp.ones((3, tests), f32)
    zero = jnp.zeros((1, tests), f32)
    test_features[...] = jnp.concatenate(
        [test_pos, test_pos, test_pos, ones] + thirds(norm(test_pos)) + [zero], axis=0
    ).astype(bf16)
    put_features(1, train_ref[...])
    wait_coords()
    put_features(0, coord_window[0])
    put_features(2, coord_window[1])
    lax.fori_loop(0, split, near_block, 0)

    for copy in copies:
        copy.wait()
    mixed_far = []
    for k in range(depth):
        mine = flows[k]
        if k:
            mine = mine + unpair(sum(received[mask, k] for mask in range(1, 1 << k)))
        other = unpair(sum(received[mask, k] for mask in range(1 << k, 2 << k)))
        mixed_far.append(triple(coupling[local + k], jnp.concatenate([mine, other], axis=0)))

    terms = jnp.zeros((depth * rank, columns), f32)
    for leaf in range(leaf_count):
        mix = jnp.concatenate(mixes[leaf] + mixed_far, axis=0)
        mix_high, mix_low = halves(mix)
        state = solved[leaf] - tn(mix_high, bases[leaf]) - tn(mix_low, bases[leaf])
        weights = state.astype(bf16)
        weight_window[leaf_count + leaf] = weights
        terms = terms + nt(bases[leaf][top:], weights)
    panel = weight_window.at[pl.ds(leaf_count, leaf_count)]
    start_weights, wait_weights = shared(
        remote(
            panel,
            weight_window.at[pl.ds(0, leaf_count)],
            weight_send.at[0],
            weight_recv.at[0],
            after,
        ),
        remote(
            panel,
            weight_window.at[pl.ds(2 * leaf_count, leaf_count)],
            weight_send.at[1],
            weight_recv.at[1],
            before,
        ),
    )
    start_weights()
    terms = terms * scale[top:]
    for k in range(depth):
        far_sent[k] = pair(terms[rows_of(k)])
    far_copies = []
    for mask in range(1, panels):
        copy = remote(
            far_sent.at[mask.bit_length() - 1],
            far_received.at[mask],
            far_send.at[mask],
            far_recv.at[mask],
            toggled(me, mask),
        )
        copy.start()
        far_copies.append(copy)
    lax.fori_loop(split, total_steps, near_block, 0)
    for copy in far_copies:
        copy.wait()
    far_rows = []
    for k in range(depth):
        far_rows.append(unpair(sum(far_received[mask] for mask in range(1 << k, 2 << k))))
    far_high, far_low = halves(jnp.concatenate(far_rows, axis=0))
    test_basis_copy.wait()
    test_basis = test_basis_ref[...].reshape(depth * rank, tests)
    wait_weights()
    held = jnp.concatenate(
        [weight_window[window_leaf(slot)] for slot in range(near)], axis=1
    )
    for tile in range(tests // TILE):
        lanes = slice(tile * TILE, (tile + 1) * TILE)
        near_sum = nn(held, blocks[:, lanes])
        far_sum = tn(far_high, test_basis[:, lanes]) + tn(far_low, test_basis[:, lanes])
        out_ref[:, lanes] = (near_sum * (1.0 / math.sqrt(near * leaf_size)) + far_sum).astype(bf16)


def shards(
    panels,
    sub_size,
    targets,
    tree_order,
    leaf_inverse,
    cluster_basis,
    coupling,
    train_coords,
    test_coords,
    test_basis,
    near_leaves,
):
    columns, points = targets.shape
    leaf_count, leaf_size = leaf_inverse.shape[0], leaf_inverse.shape[1]
    levels, rank = cluster_basis.shape[0], cluster_basis.shape[1]
    near = near_leaves.shape[1]
    tests = test_coords.shape[1]
    depth = levels - (leaf_count.bit_length() - 1)
    cross_rows = [
        sum((depth - 1 - j) * rank for j in range(b, depth - 1)) // 4 for b in range(depth - 1)
    ]
    slots = sum((1 << b) * cross_rows[b] for b in range(depth - 1))
    vmem = pl.BlockSpec(memory_space=pltpu.VMEM)
    anywhere = pl.BlockSpec(memory_space=pl.ANY)
    sems = pltpu.SemaphoreType.DMA
    operands = (
        tree_order,
        targets,
        leaf_inverse,
        cluster_basis,
        coupling,
        train_coords,
        test_coords,
        test_basis,
    )
    return pl.pallas_call(
        functools.partial(kernel, panels, sub_size),
        out_shape=jax.ShapeDtypeStruct((columns, tests), bf16),
        in_specs=[anywhere] * 9,
        out_specs=vmem,
        scratch_shapes=[pltpu.VMEM(one.shape, one.dtype) for one in operands]
        + [
            pltpu.SMEM(near_leaves.shape, near_leaves.dtype),
            pltpu.VMEM((sum(cross_rows), 4 * rank), f32),
            pltpu.VMEM((slots, 4 * rank), f32),
            pltpu.VMEM((depth, rank // 2, 2 * columns), f32),
            pltpu.VMEM((panels, depth, rank // 2, 2 * columns), f32),
            pltpu.VMEM((depth, rank // 2, 2 * columns), f32),
            pltpu.VMEM((panels, rank // 2, 2 * columns), f32),
            pltpu.VMEM((2, 3, points), bf16),
            pltpu.VMEM((3 * leaf_count, FEATS, leaf_size), bf16),
            pltpu.VMEM((FEATS, tests), bf16),
            pltpu.VMEM((near * leaf_size, tests), bf16),
            pltpu.VMEM((3 * leaf_count, columns, leaf_size), bf16),
            sems((8,)),
            sems((leaf_count,)),
            sems((panels,)),
            sems((panels,)),
            sems((panels,)),
            sems((panels,)),
            sems((panels,)),
            sems((panels,)),
            sems((2,)),
            sems((2,)),
            sems((2,)),
            sems((2,)),
        ],
        compiler_params=pltpu.CompilerParams(
            collective_id=0, has_side_effects=True, vmem_limit_bytes=60 * 1024 * 1024
        ),
    )(*operands, near_leaves)


def solution(mesh):
    return jax.shard_map(
        functools.partial(shards, mesh.shape["leaf"] * mesh.shape["sub"], mesh.shape["sub"]),
        mesh=mesh,
        in_specs=(
            P(None, ("grp", "leaf", "sub")),
            P(("grp", "leaf", "sub"), None),
            P(("grp", "leaf", "sub"), None, None),
            P(None, None, ("grp", "leaf", "sub")),
            P(("grp", "leaf", "sub"), None, None, None),
            P(None, ("grp", "leaf", "sub")),
            P(None, ("grp", "leaf", "sub")),
            P(None, None, ("grp", "leaf", "sub")),
            P(("grp", "leaf", "sub"), None),
        ),
        out_specs=P(None, ("grp", "leaf", "sub")),
        check_vma=False,
    )
```

```python
import functools
import math

import jax
import jax.numpy as jnp
from jax import lax
from jax.experimental import pallas as pl
from jax.experimental.pallas import tpu as pltpu
from jax.sharding import PartitionSpec as P

variance = 2.0
length_scale = 0.5
f32 = jnp.float32
bf16 = jnp.bfloat16
CHUNK = 256
TILE = 1024
FEATS = 16
EARLY = 4
FIRST = 5
GUARD = 2.0**-12


def nt(a, b):
    return lax.dot_general(a, b, (((1,), (1,)), ((), ())), preferred_element_type=f32)


def nn(a, b):
    return jnp.dot(a, b, preferred_element_type=f32)


def tn(a, b):
    return lax.dot_general(a, b, (((0,), (0,)), ((), ())), preferred_element_type=f32)


def halves(x):
    high = x.astype(bf16)
    return high, (x - high.astype(f32)).astype(bf16)


def thirds(x):
    first = x.astype(bf16).astype(f32)
    second = (x - first).astype(bf16).astype(f32)
    return [first, second, (x - first - second).astype(bf16).astype(f32)]


def toggled(index, mask):
    bit = 1
    while bit <= mask:
        if mask & bit:
            index = index + bit - 2 * bit * lax.rem(lax.div(index, bit), 2)
        bit *= 2
    return index


def triple(a, b):
    ah, al = halves(a)
    bh, bl = halves(b)
    return nn(ah, bh) + nn(ah, bl) + nn(al, bh)


def fold(x):
    rows = x.shape[0] // 4
    return jnp.concatenate([x[q * rows : (q + 1) * rows] for q in range(4)], axis=1)


def unfold(x):
    width = x.shape[1] // 4
    return jnp.concatenate([x[:, q * width : (q + 1) * width] for q in range(4)], axis=0)


def pair(x):
    rows = x.shape[0] // 2
    return jnp.concatenate([x[:rows], x[rows:]], axis=1)


def unpair(x):
    width = x.shape[1] // 2
    return jnp.concatenate([x[:, :width], x[:, width:]], axis=0)


def spans(depth, rank, parts):
    cross = [sum((depth - 1 - j) * rank for j in range(b, depth - 1)) // 4 for b in range(depth)]
    upper = [(depth - b) * rank // 2 for b in range(depth)]
    rows = cross if parts == "cross" else upper
    starts = [sum(rows[:b]) for b in range(depth + 1)]
    slots = [sum((1 << c) * rows[c] for c in range(b)) for b in range(depth + 1)]
    return rows, starts, slots


def kernel(
    panels,
    sub_size,
    order_hbm,
    targets_hbm,
    inverse_hbm,
    basis_hbm,
    coupling_hbm,
    train_hbm,
    test_hbm,
    test_basis_hbm,
    near_hbm,
    out_hbm,
    order_ref,
    targets_ref,
    inverse_ref,
    basis_ref,
    coupling_ref,
    train_ref,
    test_ref,
    test_basis_ref,
    near_ref,
    out_ref,
    cross_sent,
    cross_received,
    upper_sent,
    upper_received,
    sent,
    received,
    coord_window,
    features,
    test_features,
    blocks,
    pair_weights,
    side_weights,
    held,
    total,
    load_sems,
    leaf_sems,
    out_sems,
    cross_send,
    cross_recv,
    upper_send,
    upper_recv,
    round_send,
    round_recv,
    coord_send,
    coord_recv,
    pair_send,
    pair_recv,
    side_send,
    side_recv,
):
    columns, points = targets_ref.shape
    leaf_count, leaf_size = inverse_ref.shape[0], inverse_ref.shape[1]
    levels, rank = basis_ref.shape[0], basis_ref.shape[1]
    near = near_ref.shape[1]
    tests = test_ref.shape[1]
    local = leaf_count.bit_length() - 1
    depth = levels - local
    half = panels // 2
    me = lax.axis_index("leaf") * sub_size + lax.axis_index("sub")

    def load(index, source, target):
        copy = pltpu.make_async_copy(source, target, load_sems.at[index])
        copy.start()
        return copy

    basis_copy = load(0, basis_hbm, basis_ref)
    coupling_copy = load(1, coupling_hbm, coupling_ref)
    order_copy = load(2, order_hbm, order_ref)
    targets_copy = load(3, targets_hbm, targets_ref)
    leaf_copies = []
    for leaf in range(leaf_count):
        copy = pltpu.make_async_copy(
            inverse_hbm.at[leaf], inverse_ref.at[leaf], leaf_sems.at[leaf]
        )
        copy.start()
        leaf_copies.append(copy)
    train_copy = load(4, train_hbm, train_ref)
    test_copy = load(5, test_hbm, test_ref)
    near_copy = load(6, near_hbm, near_ref)
    test_basis_copy = load(7, test_basis_hbm, test_basis_ref)

    def device(index):
        return {"leaf": lax.div(index, sub_size), "sub": lax.rem(index, sub_size)}

    odd = lax.rem(me, 2)
    mate = me + 1 - 2 * odd
    side = me - 1 + 2 * odd
    has_side = (side >= 0) & (side < panels)
    side_safe = jnp.clip(side, 0, panels - 1)
    middle = (me == half - 1) | (me == half)
    greeted = list(range(1, half)) + [half]

    barrier = pltpu.get_barrier_semaphore()

    def greet(index):
        pl.semaphore_signal(
            barrier, inc=1, device_id=device(index), device_id_type=pl.DeviceIdType.MESH
        )

    @pl.when(jnp.logical_not(has_side))
    def _():
        side_weights[...] = jnp.zeros_like(side_weights)

    for mask in greeted:
        greet(toggled(me, mask))
    if panels > 2:
        pl.when(middle)(lambda: greet(side_safe))

    def remote(source, target, send, recv, index):
        return pltpu.make_async_remote_copy(
            src_ref=source,
            dst_ref=target,
            send_sem=send,
            recv_sem=recv,
            device_id=device(index),
            device_id_type=pl.DeviceIdType.MESH,
        )

    scale = jnp.concatenate(
        [jnp.full((rank, 1), 1.0 / math.sqrt(leaf_size << level), f32) for level in range(levels)],
        axis=0,
    )
    top = local * rank

    def rows_of(level):
        return slice(level * rank, (level + 1) * rank)

    def first_half(x):
        return x[:, :rank]

    def second_half(x):
        return x[:, rank:]

    basis_copy.wait()
    coupling_copy.wait()
    basis = basis_ref[...].reshape(levels * rank, points)
    coupling = [coupling_ref[0, level] for level in range(levels)]
    bases = [basis[:, leaf * leaf_size : (leaf + 1) * leaf_size] for leaf in range(leaf_count)]
    grams = [nt(one, one) for one in bases]
    gram = sum(one[top:, top:] for one in grams)
    moved = [
        scale[top:] * triple(gram[:, rows_of(k)], coupling[local + k]) for k in range(depth)
    ]
    crossing = [moved[k][(k + 1) * rank :] for k in range(depth - 1)]
    cross_rows, cross_starts, cross_slots = spans(depth, rank, "cross")
    upper_rows, upper_starts, upper_slots = spans(depth, rank, "upper")
    for b in range(depth - 1):
        parts = [second_half(crossing[b])] + [
            first_half(crossing[j]) for j in range(b + 1, depth - 1)
        ]
        cross_sent[pl.ds(cross_starts[b], cross_rows[b])] = fold(jnp.concatenate(parts, axis=0))

    def spread(b, mask, source, target, rows, starts, slots, send, recv):
        place = slots[b] + (mask - (1 << b)) * rows[b]
        copy = remote(
            source.at[pl.ds(starts[b], rows[b])],
            target.at[pl.ds(place, rows[b])],
            send.at[mask],
            recv.at[mask],
            toggled(me, mask),
        )
        copy.start()
        return copy

    def spread_upper(b, mask):
        return spread(
            b,
            mask,
            upper_sent,
            upper_received,
            upper_rows,
            upper_starts,
            upper_slots,
            upper_send,
            upper_recv,
        )

    extra = middle.astype(jnp.int32) if panels > 2 else 0
    pl.semaphore_wait(barrier, len(greeted) + extra)
    cross_copies, upper_copies = [], []
    for b in range(depth - 1):
        for mask in range(1 << b, 2 << b):
            cross_copies.append(
                spread(
                    b,
                    mask,
                    cross_sent,
                    cross_received,
                    cross_rows,
                    cross_starts,
                    cross_slots,
                    cross_send,
                    cross_recv,
                )
            )
    train_copy.wait()
    mate_coords = remote(train_ref, coord_window.at[0], coord_send.at[0], coord_recv.at[0], mate)
    side_coords = remote(
        train_ref, coord_window.at[1], coord_send.at[1], coord_recv.at[1], side_safe
    )
    mate_coords.start()
    pl.when(has_side)(side_coords.start)

    def transfer(gram, level):
        below = (level + 1) * rank
        return scale[below:] * triple(gram[below:, rows_of(level)], coupling[level])

    local_sides = []
    for level in range(local):
        width = 1 << level
        parts = [
            transfer(sum(grams[c * width + i] for i in range(width)), level)
            for c in range(leaf_count // width)
        ]
        local_sides.append(
            [first_half(parts[c]) + second_half(parts[c ^ 1]) for c in range(len(parts))]
        )

    order_copy.wait()
    targets_copy.wait()
    for copy in leaf_copies:
        copy.wait()
    near_copy.wait()
    test_copy.wait()
    stacked = jnp.concatenate(
        [targets_ref[:, h * CHUNK : (h + 1) * CHUNK] for h in range(points // CHUNK)], axis=0
    )
    order = order_ref[...]
    low, high = lax.rem(order, CHUNK), lax.div(order, CHUNK)
    solved, coefs = [], []
    for leaf in range(leaf_count):
        span = slice(leaf * leaf_size, (leaf + 1) * leaf_size)
        places = lax.broadcasted_iota(jnp.int32, (CHUNK, leaf_size), 0)
        chosen = jnp.where(places == low[:, span], 1.0, 0.0).astype(bf16)
        picked = nn(stacked, chosen)
        taken = jnp.zeros((columns, leaf_size), f32)
        for h in range(points // CHUNK):
            taken = jnp.where(
                high[:, span] == h, picked[h * columns : (h + 1) * columns], taken
            )
        state = nt(taken.astype(bf16), inverse_ref[leaf])
        state_high, state_low = halves(state)
        coefs.append((nt(bases[leaf], state_high) + nt(bases[leaf], state_low)) * scale)
        solved.append(state)

    mixes = [[] for _ in range(leaf_count)]
    for level in range(local):
        sides = local_sides[level]
        heads = [one[:rank] for one in coefs]
        for leaf in range(leaf_count):
            c = leaf >> level
            if leaf == c << level:
                mixed = triple(
                    coupling[level], jnp.concatenate([heads[c], heads[c ^ 1]], axis=0)
                )
            mixes[leaf].append(mixed)
        coefs = [
            coefs[2 * p][rank:]
            + coefs[2 * p + 1][rank:]
            - triple(sides[2 * p], heads[2 * p])
            - triple(sides[2 * p + 1], heads[2 * p + 1])
            for p in range(len(coefs) // 2)
        ]
    own = coefs[0]

    for copy in cross_copies:
        copy.wait()
    summed = []
    for b in range(depth - 1):
        flat = unfold(
            sum(
                cross_received[pl.ds(cross_slots[b] + i * cross_rows[b], cross_rows[b])]
                for i in range(1 << b)
            )
        )
        pieces, place = {}, 0
        for j in range(b, depth - 1):
            size = (depth - 1 - j) * rank
            pieces[j] = flat[place : place + size]
            place += size
        summed.append(pieces)
    rest, flows = own, []
    for j in range(depth):
        flows.append(rest[:rank])
        if j < depth - 1:
            side_sum = first_half(crossing[j]) + sum(summed[b][j] for b in range(j + 1))
            rest = rest[rank:] - triple(side_sum, flows[j])
    for k in range(depth):
        sent[k] = pair(flows[k]).astype(bf16)
    copies = []
    for mask in reversed(range(1, panels)):
        b = mask.bit_length() - 1
        copy = remote(
            sent.at[pl.ds(b, depth - b)],
            received.at[mask, pl.ds(b, depth - b)],
            round_send.at[mask],
            round_recv.at[mask],
            toggled(me, mask),
        )
        copy.start()
        copies.append(copy)
    for b in range(depth):
        parts = [moved[j][rows_of(b)] for j in range(b, depth)]
        upper_sent[pl.ds(upper_starts[b], upper_rows[b])] = pair(jnp.concatenate(parts, axis=0))
    for b in range(depth):
        for mask in range(1 << b, 2 << b):
            upper_copies.append(spread_upper(b, mask))

    gain = 3.0 / (length_scale * length_scale) * math.log2(math.e) ** 2

    def norm(pos):
        return gain * (pos[0:1] * pos[0:1] + pos[1:2] * pos[1:2] + pos[2:3] * pos[2:3])

    def train_side(pos):
        ones = jnp.ones((3, points), f32)
        zero = jnp.zeros((1, points), f32)
        parts = thirds(-2.0 * gain * pos) + thirds(norm(pos)) + [ones, zero + GUARD]
        return jnp.concatenate(parts, axis=0).astype(bf16)

    def put_features(panel, pos):
        made = train_side(pos.astype(f32))
        for leaf in range(leaf_count):
            features[panel * leaf_count + leaf] = made[:, leaf * leaf_size : (leaf + 1) * leaf_size]

    test_pos = test_ref[...].astype(f32)
    ones = jnp.ones((3, tests), f32)
    zero = jnp.zeros((1, tests), f32)
    test_features[...] = jnp.concatenate(
        [test_pos, test_pos, test_pos, ones] + thirds(norm(test_pos)) + [zero + 1.0], axis=0
    ).astype(bf16)
    put_features(0, train_ref[...])
    for leaf in range(leaf_count):
        mix_high, mix_low = halves(jnp.concatenate(mixes[leaf], axis=0))
        solved[leaf] = (
            solved[leaf] - tn(mix_high, bases[leaf][:top]) - tn(mix_low, bases[leaf][:top])
        )

    def within(place):
        return jnp.clip(place + 1, 0, 1) * jnp.clip(leaf_count - place, 0, 1)

    def window_leaf(slot):
        leaf_id = near_ref[0, slot]
        in_own = leaf_id - me * leaf_count
        in_mate = leaf_id - mate * leaf_count
        in_side = jnp.clip(leaf_id - side * leaf_count, 0, leaf_count - 1)
        is_own, is_mate = within(in_own), within(in_mate)
        return (
            is_own * in_own
            + is_mate * (leaf_count + in_mate)
            + (1 - is_own - is_mate) * (2 * leaf_count + in_side)
        )

    def kept(weights, flag):
        return (weights.astype(f32) * flag.astype(f32)).astype(bf16)

    tiles = tests // TILE

    def near_block(slot, carry):
        squared = tn(features[window_leaf(slot)], test_features[...])
        scaled = squared * lax.rsqrt(squared)
        value = (scaled + 1.0 / math.log(2.0)) * jnp.exp2(
            math.log2(variance * math.log(2.0)) - scaled
        )
        blocks[slot] = value.astype(bf16)
        return carry

    def add_block(slot):
        total[...] = total[...] + nn(held[slot], blocks[slot])

    early = near * EARLY // 8
    first = near * FIRST // 8

    mate_coords.wait()
    put_features(1, coord_window[0])
    pl.when(has_side)(side_coords.wait)
    put_features(2, coord_window[1])
    lax.fori_loop(0, early, near_block, 0)

    for copy in copies:
        copy.wait()
    mines, others, mixed_far = [], [], []
    for k in range(depth):
        mine = flows[k]
        if k:
            mine = mine + unpair(sum(received[mask, k].astype(f32) for mask in range(1, 1 << k)))
        other = unpair(sum(received[mask, k].astype(f32) for mask in range(1 << k, 2 << k)))
        mines.append(mine)
        others.append(other)
        mixed_far.append(triple(coupling[local + k], jnp.concatenate([mine, other], axis=0)))

    far_mix_high, far_mix_low = halves(jnp.concatenate(mixed_far, axis=0))
    side_copies = []
    for leaf in range(leaf_count):
        upper_basis = bases[leaf][top:]
        state = solved[leaf] - tn(far_mix_high, upper_basis) - tn(far_mix_low, upper_basis)
        pair_weights[leaf] = state.astype(bf16)
        copy = remote(
            pair_weights.at[leaf],
            side_weights.at[leaf],
            side_send.at[leaf],
            side_recv.at[leaf],
            side_safe,
        )
        pl.when(has_side)(copy.start)
        side_copies.append(copy)
    mate_weights = remote(
        pair_weights.at[pl.ds(0, leaf_count)],
        pair_weights.at[pl.ds(leaf_count, leaf_count)],
        pair_send.at[0],
        pair_recv.at[0],
        mate,
    )
    mate_weights.start()

    lax.fori_loop(early, first, near_block, 0)
    for copy in upper_copies:
        copy.wait()
    far_rows = []
    for b in range(depth):
        flat = unpair(
            sum(
                upper_received[pl.ds(upper_slots[b] + i * upper_rows[b], upper_rows[b])]
                for i in range(1 << b)
            )
        )
        row = others[b]
        for j in range(b, depth):
            joined = [others[j], mines[j]] if j == b else [mines[j], others[j]]
            row = row - triple(flat[rows_of(j - b)], jnp.concatenate(joined, axis=0))
        far_rows.append(row)
    far_high, far_low = halves(jnp.concatenate(far_rows, axis=0))
    test_basis_copy.wait()
    test_basis = test_basis_ref[...].reshape(depth * rank, tests)
    weigh = math.sqrt(near * leaf_size)
    for tile in range(tiles):
        lanes = slice(tile * TILE, (tile + 1) * TILE)
        total[:, lanes] = weigh * (
            tn(far_high, test_basis[:, lanes]) + tn(far_low, test_basis[:, lanes])
        )
    mate_weights.wait()
    for slot in range(near):
        index = window_leaf(slot)
        weights = pair_weights[jnp.minimum(index, 2 * leaf_count - 1)]
        held[slot] = kept(weights, jnp.clip(2 * leaf_count - index, 0, 1))

    added = 0
    for slot in range(first, near):
        upto = max(min(added + 2, slot), 0)
        for done in range(added, upto):
            add_block(done)
        added = upto
        near_block(slot, 0)
    for slot in range(added, near):
        add_block(slot)

    places, arrived = [], []
    for leaf in range(leaf_count):
        pl.when(has_side)(side_copies[leaf].wait)
    for leaf in range(leaf_count):
        found, where = 0, 0
        for slot in range(near):
            away = window_leaf(slot) - 2 * leaf_count - leaf
            match = jnp.clip(1 - away * away, 0, 1)
            found = found + match
            where = where + match * slot
        arrived.append(kept(side_weights[leaf], jnp.clip(found, 0, 1)))
        places.append(jnp.clip(where, 0, near - 1))
    out_copies = []
    for tile in range(tiles):
        lanes = slice(tile * TILE, (tile + 1) * TILE)
        value = total[:, lanes]
        for weights, where in zip(arrived, places):
            value = value + nn(weights, blocks[where, :, lanes])
        out_ref[:, lanes] = (value * (1.0 / weigh)).astype(bf16)
        copy = pltpu.make_async_copy(out_ref.at[:, lanes], out_hbm.at[:, lanes], out_sems.at[tile])
        copy.start()
        out_copies.append(copy)
    for copy in out_copies:
        copy.wait()


def shards(
    panels,
    sub_size,
    targets,
    tree_order,
    leaf_inverse,
    cluster_basis,
    coupling,
    train_coords,
    test_coords,
    test_basis,
    near_leaves,
):
    columns, points = targets.shape
    leaf_count, leaf_size = leaf_inverse.shape[0], leaf_inverse.shape[1]
    levels, rank = cluster_basis.shape[0], cluster_basis.shape[1]
    near = near_leaves.shape[1]
    tests = test_coords.shape[1]
    depth = levels - (leaf_count.bit_length() - 1)
    cross_starts, cross_slots = spans(depth, rank, "cross")[1:]
    upper_starts, upper_slots = spans(depth, rank, "upper")[1:]
    anywhere = pl.BlockSpec(memory_space=pl.ANY)
    sems = pltpu.SemaphoreType.DMA
    operands = (
        tree_order,
        targets,
        leaf_inverse,
        cluster_basis,
        coupling,
        train_coords,
        test_coords,
        test_basis,
    )
    return pl.pallas_call(
        functools.partial(kernel, panels, sub_size),
        out_shape=jax.ShapeDtypeStruct((columns, tests), bf16),
        in_specs=[anywhere] * 9,
        out_specs=anywhere,
        scratch_shapes=[pltpu.VMEM(one.shape, one.dtype) for one in operands]
        + [
            pltpu.SMEM(near_leaves.shape, near_leaves.dtype),
            pltpu.VMEM((columns, tests), bf16),
            pltpu.VMEM((cross_starts[-1], 4 * rank), f32),
            pltpu.VMEM((cross_slots[-1], 4 * rank), f32),
            pltpu.VMEM((upper_starts[-1], 4 * rank), f32),
            pltpu.VMEM((upper_slots[-1], 4 * rank), f32),
            pltpu.VMEM((depth, rank // 2, 2 * columns), bf16),
            pltpu.VMEM((panels, depth, rank // 2, 2 * columns), bf16),
            pltpu.VMEM((2, 3, points), bf16),
            pltpu.VMEM((3 * leaf_count, FEATS, leaf_size), bf16),
            pltpu.VMEM((FEATS, tests), bf16),
            pltpu.VMEM((near, leaf_size, tests), bf16),
            pltpu.VMEM((2 * leaf_count, columns, leaf_size), bf16),
            pltpu.VMEM((leaf_count, columns, leaf_size), bf16),
            pltpu.VMEM((near, columns, leaf_size), bf16),
            pltpu.VMEM((columns, tests), f32),
            sems((8,)),
            sems((leaf_count,)),
            sems((tests // TILE,)),
            sems((panels,)),
            sems((panels,)),
            sems((panels,)),
            sems((panels,)),
            sems((panels,)),
            sems((panels,)),
            sems((2,)),
            sems((2,)),
            sems((1,)),
            sems((1,)),
            sems((leaf_count,)),
            sems((leaf_count,)),
        ],
        compiler_params=pltpu.CompilerParams(
            collective_id=0, has_side_effects=True, vmem_limit_bytes=60 * 1024 * 1024
        ),
    )(*operands, near_leaves)


def solution(mesh):
    return jax.shard_map(
        functools.partial(shards, mesh.shape["leaf"] * mesh.shape["sub"], mesh.shape["sub"]),
        mesh=mesh,
        in_specs=(
            P(None, ("grp", "leaf", "sub")),
            P(("grp", "leaf", "sub"), None),
            P(("grp", "leaf", "sub"), None, None),
            P(None, None, ("grp", "leaf", "sub")),
            P(("grp", "leaf", "sub"), None, None, None),
            P(None, ("grp", "leaf", "sub")),
            P(None, ("grp", "leaf", "sub")),
            P(None, None, ("grp", "leaf", "sub")),
            P(("grp", "leaf", "sub"), None),
        ),
        out_specs=P(None, ("grp", "leaf", "sub")),
        check_vma=False,
    )
```

```python
import functools
import math

import jax
import jax.numpy as jnp
from jax import lax
from jax.experimental import pallas as pl
from jax.experimental.pallas import tpu as pltpu
from jax.sharding import PartitionSpec as P

variance = 2.0
length_scale = 0.5
f32 = jnp.float32
bf16 = jnp.bfloat16
CHUNK = 256
TILE = 1024
FEATS = 16
EARLY = 4
MIDDLE = 7
GUARD = 2.0**-12


def nt(a, b):
    return lax.dot_general(a, b, (((1,), (1,)), ((), ())), preferred_element_type=f32)


def nn(a, b):
    return jnp.dot(a, b, preferred_element_type=f32)


def tn(a, b):
    return lax.dot_general(a, b, (((0,), (0,)), ((), ())), preferred_element_type=f32)


def halves(x):
    high = x.astype(bf16)
    return high, (x - high.astype(f32)).astype(bf16)


def thirds(x):
    first = x.astype(bf16).astype(f32)
    second = (x - first).astype(bf16).astype(f32)
    return [first, second, (x - first - second).astype(bf16).astype(f32)]


def toggled(index, mask):
    bit = 1
    while bit <= mask:
        if mask & bit:
            index = index + bit - 2 * bit * lax.rem(lax.div(index, bit), 2)
        bit *= 2
    return index


def triple(a, b):
    ah, al = halves(a)
    bh, bl = halves(b)
    return nn(ah, bh) + nn(ah, bl) + nn(al, bh)


def fold(x):
    rows = x.shape[0] // 4
    return jnp.concatenate([x[q * rows : (q + 1) * rows] for q in range(4)], axis=1)


def unfold(x):
    width = x.shape[1] // 4
    return jnp.concatenate([x[:, q * width : (q + 1) * width] for q in range(4)], axis=0)


def pair(x):
    rows = x.shape[0] // 2
    return jnp.concatenate([x[:rows], x[rows:]], axis=1)


def unpair(x):
    width = x.shape[1] // 2
    return jnp.concatenate([x[:, :width], x[:, width:]], axis=0)


def spans(depth, rank, parts):
    cross = [sum((depth - 1 - j) * rank for j in range(b, depth - 1)) // 4 for b in range(depth)]
    upper = [(depth - b) * rank // 2 for b in range(depth)]
    rows = cross if parts == "cross" else upper
    starts = [sum(rows[:b]) for b in range(depth + 1)]
    slots = [sum((1 << c) * rows[c] for c in range(b)) for b in range(depth + 1)]
    return rows, starts, slots


def kernel(
    panels,
    sub_size,
    order_hbm,
    targets_hbm,
    inverse_hbm,
    basis_hbm,
    coupling_hbm,
    train_hbm,
    test_hbm,
    test_basis_hbm,
    near_hbm,
    out_hbm,
    order_ref,
    targets_ref,
    inverse_ref,
    basis_ref,
    coupling_ref,
    train_ref,
    test_ref,
    test_basis_ref,
    near_ref,
    out_ref,
    cross_sent,
    cross_received,
    upper_sent,
    upper_received,
    sent,
    received,
    coord_window,
    features,
    test_features,
    blocks,
    weight_window,
    load_sems,
    out_sems,
    cross_send,
    cross_recv,
    upper_send,
    upper_recv,
    round_send,
    round_recv,
    coord_send,
    coord_recv,
    pair_send,
    pair_recv,
    side_send,
    side_recv,
):
    columns, points = targets_ref.shape
    leaf_count, leaf_size = inverse_ref.shape[0], inverse_ref.shape[1]
    levels, rank = basis_ref.shape[0], basis_ref.shape[1]
    near = near_ref.shape[1]
    tests = test_ref.shape[1]
    local = leaf_count.bit_length() - 1
    depth = levels - local
    half = panels // 2
    me = lax.axis_index("leaf") * sub_size + lax.axis_index("sub")

    def load(index, source, target):
        copy = pltpu.make_async_copy(source, target, load_sems.at[index])
        copy.start()
        return copy

    basis_copy = load(0, basis_hbm, basis_ref)
    coupling_copy = load(1, coupling_hbm, coupling_ref)
    order_copy = load(2, order_hbm, order_ref)
    targets_copy = load(3, targets_hbm, targets_ref)
    inverse_copy = load(8, inverse_hbm, inverse_ref)
    train_copy = load(4, train_hbm, train_ref)
    test_copy = load(5, test_hbm, test_ref)
    near_copy = load(6, near_hbm, near_ref)
    test_basis_copy = load(7, test_basis_hbm, test_basis_ref)

    def device(index):
        return {"leaf": lax.div(index, sub_size), "sub": lax.rem(index, sub_size)}

    odd = lax.rem(me, 2)
    mate = me + 1 - 2 * odd
    side = me - 1 + 2 * odd
    has_side = (side >= 0) & (side < panels)
    side_safe = jnp.clip(side, 0, panels - 1)
    middle = (me == half - 1) | (me == half)
    greeted = list(range(1, half)) + [half]

    barrier = pltpu.get_barrier_semaphore()

    def greet(index):
        pl.semaphore_signal(
            barrier, inc=1, device_id=device(index), device_id_type=pl.DeviceIdType.MESH
        )

    for mask in greeted:
        greet(toggled(me, mask))
    if panels > 2:
        pl.when(middle)(lambda: greet(side_safe))

    def remote(source, target, send, recv, index):
        return pltpu.make_async_remote_copy(
            src_ref=source,
            dst_ref=target,
            send_sem=send,
            recv_sem=recv,
            device_id=device(index),
            device_id_type=pl.DeviceIdType.MESH,
        )

    scale = jnp.concatenate(
        [jnp.full((rank, 1), 1.0 / math.sqrt(leaf_size << level), f32) for level in range(levels)],
        axis=0,
    )
    top = local * rank

    def rows_of(level):
        return slice(level * rank, (level + 1) * rank)

    def first_half(x):
        return x[:, :rank]

    def second_half(x):
        return x[:, rank:]

    basis_copy.wait()
    coupling_copy.wait()
    basis = basis_ref[...].reshape(levels * rank, points)
    coupling = [coupling_ref[0, level] for level in range(levels)]
    bases = [basis[:, leaf * leaf_size : (leaf + 1) * leaf_size] for leaf in range(leaf_count)]
    grams = [nt(one, one) for one in bases]
    gram = sum(one[top:, top:] for one in grams)
    moved = [
        scale[top:] * triple(gram[:, rows_of(k)], coupling[local + k]) for k in range(depth)
    ]
    crossing = [moved[k][(k + 1) * rank :] for k in range(depth - 1)]
    cross_rows, cross_starts, cross_slots = spans(depth, rank, "cross")
    upper_rows, upper_starts, upper_slots = spans(depth, rank, "upper")
    for b in range(depth - 1):
        parts = [second_half(crossing[b])] + [
            first_half(crossing[j]) for j in range(b + 1, depth - 1)
        ]
        cross_sent[pl.ds(cross_starts[b], cross_rows[b])] = fold(jnp.concatenate(parts, axis=0))

    def spread(b, mask, source, target, rows, starts, slots, send, recv):
        place = slots[b] + (mask - (1 << b)) * rows[b]
        remote(
            source.at[pl.ds(starts[b], rows[b])],
            target.at[pl.ds(place, rows[b])],
            send.at[0],
            recv.at[0],
            toggled(me, mask),
        ).start()

    def spread_upper(b, mask):
        spread(
            b,
            mask,
            upper_sent,
            upper_received,
            upper_rows,
            upper_starts,
            upper_slots,
            upper_send,
            upper_recv,
        )

    extra = middle.astype(jnp.int32) if panels > 2 else 0
    pl.semaphore_wait(barrier, len(greeted) + extra)
    for b in range(depth - 1):
        for mask in range(1 << b, 2 << b):
            spread(
                b,
                mask,
                cross_sent,
                cross_received,
                cross_rows,
                cross_starts,
                cross_slots,
                cross_send,
                cross_recv,
            )
    train_copy.wait()
    mate_coords = remote(train_ref, coord_window.at[0], coord_send.at[0], coord_recv.at[0], mate)
    side_coords = remote(
        train_ref, coord_window.at[1], coord_send.at[1], coord_recv.at[1], side_safe
    )
    mate_coords.start()
    pl.when(has_side)(side_coords.start)

    def transfer(gram, level):
        below = (level + 1) * rank
        return scale[below:] * triple(gram[below:, rows_of(level)], coupling[level])

    local_sides = []
    for level in range(local):
        width = 1 << level
        parts = [
            transfer(sum(grams[c * width + i] for i in range(width)), level)
            for c in range(leaf_count // width)
        ]
        local_sides.append(
            [first_half(parts[c]) + second_half(parts[c ^ 1]) for c in range(len(parts))]
        )

    order_copy.wait()
    targets_copy.wait()
    inverse_copy.wait()
    near_copy.wait()
    test_copy.wait()
    stacked = jnp.concatenate(
        [targets_ref[:, h * CHUNK : (h + 1) * CHUNK] for h in range(points // CHUNK)], axis=0
    )
    order = order_ref[...]
    low, high = lax.rem(order, CHUNK), lax.div(order, CHUNK)
    solved, coefs = [], []
    for leaf in range(leaf_count):
        span = slice(leaf * leaf_size, (leaf + 1) * leaf_size)
        places = lax.broadcasted_iota(jnp.int32, (CHUNK, leaf_size), 0)
        chosen = jnp.where(places == low[:, span], 1.0, 0.0).astype(bf16)
        picked = nn(stacked, chosen)
        taken = jnp.zeros((columns, leaf_size), f32)
        for h in range(points // CHUNK):
            taken = jnp.where(
                high[:, span] == h, picked[h * columns : (h + 1) * columns], taken
            )
        state = nt(taken.astype(bf16), inverse_ref[leaf])
        state_high, state_low = halves(state)
        coefs.append((nt(bases[leaf], state_high) + nt(bases[leaf], state_low)) * scale)
        solved.append(state)

    mixes = [[] for _ in range(leaf_count)]
    for level in range(local):
        sides = local_sides[level]
        heads = [one[:rank] for one in coefs]
        for leaf in range(leaf_count):
            c = leaf >> level
            if leaf == c << level:
                mixed = triple(
                    coupling[level], jnp.concatenate([heads[c], heads[c ^ 1]], axis=0)
                )
            mixes[leaf].append(mixed)
        coefs = [
            coefs[2 * p][rank:]
            + coefs[2 * p + 1][rank:]
            - triple(sides[2 * p], heads[2 * p])
            - triple(sides[2 * p + 1], heads[2 * p + 1])
            for p in range(len(coefs) // 2)
        ]
    own = coefs[0]

    remote(cross_received, cross_received, cross_send.at[0], cross_recv.at[0], mate).wait()
    summed = []
    for b in range(depth - 1):
        flat = unfold(
            sum(
                cross_received[pl.ds(cross_slots[b] + i * cross_rows[b], cross_rows[b])]
                for i in range(1 << b)
            )
        )
        pieces, place = {}, 0
        for j in range(b, depth - 1):
            size = (depth - 1 - j) * rank
            pieces[j] = flat[place : place + size]
            place += size
        summed.append(pieces)
    rest, flows = own, []
    for j in range(depth):
        flows.append(rest[:rank])
        if j < depth - 1:
            side_sum = first_half(crossing[j]) + sum(summed[b][j] for b in range(j + 1))
            rest = rest[rank:] - triple(side_sum, flows[j])
    for k in range(depth):
        sent[k] = pair(flows[k])
    unit_starts, units = [0], 0
    for mask in range(1, panels):
        unit_starts.append(units)
        units += depth - (mask.bit_length() - 1)
    for mask in reversed(range(1, panels)):
        b = mask.bit_length() - 1
        remote(
            sent.at[pl.ds(b, depth - b)],
            received.at[pl.ds(unit_starts[mask], depth - b)],
            round_send.at[0],
            round_recv.at[0],
            toggled(me, mask),
        ).start()
    for b in range(depth):
        parts = [moved[j][rows_of(b)] for j in range(b, depth)]
        upper_sent[pl.ds(upper_starts[b], upper_rows[b])] = pair(
            jnp.concatenate(parts, axis=0)
        ).astype(bf16)
    for b in range(depth):
        for mask in range(1 << b, 2 << b):
            spread_upper(b, mask)

    gain = 3.0 / (length_scale * length_scale) * math.log2(math.e) ** 2

    def norm(pos):
        return gain * (pos[0:1] * pos[0:1] + pos[1:2] * pos[1:2] + pos[2:3] * pos[2:3])

    def train_side(pos):
        ones = jnp.ones((3, points), f32)
        zero = jnp.zeros((1, points), f32)
        parts = thirds(-2.0 * gain * pos) + thirds(norm(pos)) + [ones, zero + GUARD]
        return jnp.concatenate(parts, axis=0).astype(bf16)

    def put_features(panel, pos):
        made = train_side(pos.astype(f32))
        for leaf in range(leaf_count):
            features[panel * leaf_count + leaf] = made[:, leaf * leaf_size : (leaf + 1) * leaf_size]

    test_pos = test_ref[...].astype(f32)
    ones = jnp.ones((3, tests), f32)
    zero = jnp.zeros((1, tests), f32)
    test_features[...] = jnp.concatenate(
        [test_pos, test_pos, test_pos, ones] + thirds(norm(test_pos)) + [zero + 1.0], axis=0
    ).astype(bf16)
    put_features(0, train_ref[...])
    for leaf in range(leaf_count):
        mix_high, mix_low = halves(jnp.concatenate(mixes[leaf], axis=0))
        solved[leaf] = (
            solved[leaf] - tn(mix_high, bases[leaf][:top]) - tn(mix_low, bases[leaf][:top])
        )

    def within(place):
        return jnp.clip(place + 1, 0, 1) * jnp.clip(leaf_count - place, 0, 1)

    def window_leaf(slot):
        leaf_id = near_ref[0, slot]
        in_own = leaf_id - me * leaf_count
        in_mate = leaf_id - mate * leaf_count
        in_side = jnp.clip(leaf_id - side * leaf_count, 0, leaf_count - 1)
        is_own, is_mate = within(in_own), within(in_mate)
        return (
            is_own * in_own
            + is_mate * (leaf_count + in_mate)
            + (1 - is_own - is_mate) * (2 * leaf_count + in_side)
        )

    tiles = tests // TILE

    def near_block(slot, carry):
        squared = tn(features[window_leaf(slot)], test_features[...])
        scaled = squared * lax.rsqrt(squared)
        value = (scaled + 1.0 / math.log(2.0)) * jnp.exp2(
            math.log2(variance * math.log(2.0)) - scaled
        )
        rows = pl.ds(pl.multiple_of(slot * leaf_size, leaf_size), leaf_size)
        blocks[rows] = value.astype(bf16)
        return carry

    early = near * EARLY // 8
    middle_slot = near * MIDDLE // 8

    mate_coords.wait()
    put_features(1, coord_window[0])
    pl.when(has_side)(side_coords.wait)
    put_features(2, coord_window[1])
    lax.fori_loop(0, early, near_block, 0)

    remote(received, received, round_send.at[0], round_recv.at[0], mate).wait()
    mines, others, mixed_far = [], [], []

    def gathered(masks, k):
        return unpair(
            sum(received[unit_starts[mask] + k - (mask.bit_length() - 1)] for mask in masks)
        )

    for k in range(depth):
        mine = flows[k]
        if k:
            mine = mine + gathered(range(1, 1 << k), k)
        other = gathered(range(1 << k, 2 << k), k)
        mines.append(mine)
        others.append(other)
        mixed_far.append(triple(coupling[local + k], jnp.concatenate([mine, other], axis=0)))

    far_mix_high, far_mix_low = halves(jnp.concatenate(mixed_far, axis=0))
    for leaf in range(leaf_count):
        upper_basis = bases[leaf][top:]
        state = solved[leaf] - tn(far_mix_high, upper_basis) - tn(far_mix_low, upper_basis)
        weight_window[leaf] = state.astype(bf16)
        copy = remote(
            weight_window.at[leaf],
            weight_window.at[2 * leaf_count + leaf],
            side_send.at[0],
            side_recv.at[0],
            side_safe,
        )
        pl.when(has_side)(copy.start)

    def panel_of(index):
        return weight_window.at[pl.ds(index * leaf_count, leaf_count)]

    mate_weights = remote(panel_of(0), panel_of(1), pair_send.at[0], pair_recv.at[0], mate)
    mate_weights.start()
    side_weights = remote(panel_of(0), panel_of(2), side_send.at[0], side_recv.at[0], side_safe)

    lax.fori_loop(early, middle_slot, near_block, 0)
    remote(upper_received, upper_received, upper_send.at[0], upper_recv.at[0], mate).wait()
    far_rows = []
    for b in range(depth):
        flat = unpair(
            sum(
                upper_received[pl.ds(upper_slots[b] + i * upper_rows[b], upper_rows[b])].astype(f32)
                for i in range(1 << b)
            )
        )
        row = others[b]
        for j in range(b, depth):
            joined = [others[j], mines[j]] if j == b else [mines[j], others[j]]
            row = row - triple(flat[rows_of(j - b)], jnp.concatenate(joined, axis=0))
        far_rows.append(row)
    far_high, far_low = halves(jnp.concatenate(far_rows, axis=0))
    test_basis_copy.wait()
    test_basis = test_basis_ref[...].reshape(depth * rank, tests)
    lax.fori_loop(middle_slot, near, near_block, 0)

    mate_weights.wait()
    pl.when(has_side)(side_weights.wait)
    held = jnp.concatenate([weight_window[window_leaf(slot)] for slot in range(near)], axis=1)
    for tile in range(tiles):
        lanes = slice(tile * TILE, (tile + 1) * TILE)
        far_sum = tn(far_high, test_basis[:, lanes]) + tn(far_low, test_basis[:, lanes])
        near_sum = nn(held, blocks[:, lanes])
        out_ref[:, lanes] = (near_sum * (1.0 / math.sqrt(near * leaf_size)) + far_sum).astype(bf16)
        pltpu.make_async_copy(
            out_ref.at[:, lanes], out_hbm.at[:, lanes], out_sems.at[0]
        ).start()
    pltpu.make_async_copy(out_ref, out_hbm, out_sems.at[0]).wait()


def shards(
    panels,
    sub_size,
    targets,
    tree_order,
    leaf_inverse,
    cluster_basis,
    coupling,
    train_coords,
    test_coords,
    test_basis,
    near_leaves,
):
    columns, points = targets.shape
    leaf_count, leaf_size = leaf_inverse.shape[0], leaf_inverse.shape[1]
    levels, rank = cluster_basis.shape[0], cluster_basis.shape[1]
    near = near_leaves.shape[1]
    tests = test_coords.shape[1]
    depth = levels - (leaf_count.bit_length() - 1)
    cross_starts, cross_slots = spans(depth, rank, "cross")[1:]
    upper_starts, upper_slots = spans(depth, rank, "upper")[1:]
    units = sum((depth - b) << b for b in range(depth))
    anywhere = pl.BlockSpec(memory_space=pl.ANY)
    sems = pltpu.SemaphoreType.DMA
    operands = (
        tree_order,
        targets,
        leaf_inverse,
        cluster_basis,
        coupling,
        train_coords,
        test_coords,
        test_basis,
    )
    return pl.pallas_call(
        functools.partial(kernel, panels, sub_size),
        out_shape=jax.ShapeDtypeStruct((columns, tests), bf16),
        in_specs=[anywhere] * 9,
        out_specs=anywhere,
        scratch_shapes=[pltpu.VMEM(one.shape, one.dtype) for one in operands]
        + [
            pltpu.SMEM(near_leaves.shape, near_leaves.dtype),
            pltpu.VMEM((columns, tests), bf16),
            pltpu.VMEM((cross_starts[-1], 4 * rank), f32),
            pltpu.VMEM((cross_slots[-1], 4 * rank), f32),
            pltpu.VMEM((upper_starts[-1], 4 * rank), bf16),
            pltpu.VMEM((upper_slots[-1], 4 * rank), bf16),
            pltpu.VMEM((depth, rank // 2, 2 * columns), f32),
            pltpu.VMEM((units, rank // 2, 2 * columns), f32),
            pltpu.VMEM((2, 3, points), bf16),
            pltpu.VMEM((3 * leaf_count, FEATS, leaf_size), bf16),
            pltpu.VMEM((FEATS, tests), bf16),
            pltpu.VMEM((near * leaf_size, tests), bf16),
            pltpu.VMEM((3 * leaf_count, columns, leaf_size), bf16),
            sems((9,)),
            sems((1,)),
            sems((1,)),
            sems((1,)),
            sems((1,)),
            sems((1,)),
            sems((1,)),
            sems((1,)),
            sems((2,)),
            sems((2,)),
            sems((1,)),
            sems((1,)),
            sems((1,)),
            sems((1,)),
        ],
        compiler_params=pltpu.CompilerParams(
            collective_id=0, has_side_effects=True, vmem_limit_bytes=60 * 1024 * 1024
        ),
    )(*operands, near_leaves)


def solution(mesh):
    return jax.shard_map(
        functools.partial(shards, mesh.shape["leaf"] * mesh.shape["sub"], mesh.shape["sub"]),
        mesh=mesh,
        in_specs=(
            P(None, ("grp", "leaf", "sub")),
            P(("grp", "leaf", "sub"), None),
            P(("grp", "leaf", "sub"), None, None),
            P(None, None, ("grp", "leaf", "sub")),
            P(("grp", "leaf", "sub"), None, None, None),
            P(None, ("grp", "leaf", "sub")),
            P(None, ("grp", "leaf", "sub")),
            P(None, None, ("grp", "leaf", "sub")),
            P(("grp", "leaf", "sub"), None),
        ),
        out_specs=P(None, ("grp", "leaf", "sub")),
        check_vma=False,
    )
```

```python
import functools
import math

import jax
import jax.numpy as jnp
from jax import lax
from jax.experimental import pallas as pl
from jax.experimental.pallas import tpu as pltpu
from jax.sharding import PartitionSpec as P

variance = 2.0
length_scale = 0.5
f32 = jnp.float32
bf16 = jnp.bfloat16
CHUNK = 256
TILE = 1024
FEATS = 16
EARLY = 4
MIDDLE = 6
GUARD = 2.0**-12


def nt(a, b):
    return lax.dot_general(a, b, (((1,), (1,)), ((), ())), preferred_element_type=f32)


def nn(a, b):
    return jnp.dot(a, b, preferred_element_type=f32)


def tn(a, b):
    return lax.dot_general(a, b, (((0,), (0,)), ((), ())), preferred_element_type=f32)


def halves(x):
    high = x.astype(bf16)
    return high, (x - high.astype(f32)).astype(bf16)


def thirds(x):
    first = x.astype(bf16).astype(f32)
    second = (x - first).astype(bf16).astype(f32)
    return [first, second, (x - first - second).astype(bf16).astype(f32)]


def toggled(index, mask):
    bit = 1
    while bit <= mask:
        if mask & bit:
            index = index + bit - 2 * bit * lax.rem(lax.div(index, bit), 2)
        bit *= 2
    return index


def triple(a, b):
    ah, al = halves(a)
    bh, bl = halves(b)
    return nn(ah, bh) + nn(ah, bl) + nn(al, bh)


def fold(x):
    rows = x.shape[0] // 4
    return jnp.concatenate([x[q * rows : (q + 1) * rows] for q in range(4)], axis=1)


def unfold(x):
    width = x.shape[1] // 4
    return jnp.concatenate([x[:, q * width : (q + 1) * width] for q in range(4)], axis=0)


def pair(x):
    rows = x.shape[0] // 2
    return jnp.concatenate([x[:rows], x[rows:]], axis=1)


def unpair(x):
    width = x.shape[1] // 2
    return jnp.concatenate([x[:, :width], x[:, width:]], axis=0)


def spans(depth, rank, parts):
    cross = [sum((depth - 1 - j) * rank for j in range(b, depth - 1)) // 4 for b in range(depth)]
    upper = [(depth - b) * rank // 2 for b in range(depth)]
    rows = cross if parts == "cross" else upper
    starts = [sum(rows[:b]) for b in range(depth + 1)]
    slots = [sum((1 << c) * rows[c] for c in range(b)) for b in range(depth + 1)]
    return rows, starts, slots


def kernel(
    panels,
    sub_size,
    order_hbm,
    targets_hbm,
    inverse_hbm,
    basis_hbm,
    coupling_hbm,
    train_hbm,
    test_hbm,
    test_basis_hbm,
    near_hbm,
    out_hbm,
    order_ref,
    targets_ref,
    inverse_ref,
    basis_ref,
    coupling_ref,
    train_ref,
    test_ref,
    test_basis_ref,
    near_ref,
    out_ref,
    cross_sent,
    cross_received,
    upper_sent,
    upper_received,
    sent,
    received,
    coord_window,
    features,
    test_features,
    blocks,
    weight_window,
    far_sum,
    load_sems,
    out_sems,
    cross_send,
    cross_recv,
    upper_send,
    upper_recv,
    round_send,
    round_recv,
    coord_send,
    coord_recv,
    pair_send,
    pair_recv,
    side_send,
    side_recv,
):
    columns, points = targets_ref.shape
    leaf_count, leaf_size = inverse_ref.shape[0], inverse_ref.shape[1]
    levels, rank = basis_ref.shape[0], basis_ref.shape[1]
    near = near_ref.shape[1]
    tests = test_ref.shape[1]
    local = leaf_count.bit_length() - 1
    depth = levels - local
    half = panels // 2
    me = lax.axis_index("leaf") * sub_size + lax.axis_index("sub")

    def load(index, source, target):
        copy = pltpu.make_async_copy(source, target, load_sems.at[index])
        copy.start()
        return copy

    basis_copy = load(0, basis_hbm, basis_ref)
    coupling_copy = load(1, coupling_hbm, coupling_ref)
    order_copy = load(2, order_hbm, order_ref)
    targets_copy = load(3, targets_hbm, targets_ref)
    inverse_copy = load(8, inverse_hbm, inverse_ref)
    train_copy = load(4, train_hbm, train_ref)
    test_copy = load(5, test_hbm, test_ref)
    near_copy = load(6, near_hbm, near_ref)
    test_basis_copy = load(7, test_basis_hbm, test_basis_ref)

    def device(index):
        return {"leaf": lax.div(index, sub_size), "sub": lax.rem(index, sub_size)}

    odd = lax.rem(me, 2)
    mate = me + 1 - 2 * odd
    side = me - 1 + 2 * odd
    has_side = (side >= 0) & (side < panels)
    side_safe = jnp.clip(side, 0, panels - 1)
    middle = (me == half - 1) | (me == half)
    greeted = list(range(1, half)) + [half]

    barrier = pltpu.get_barrier_semaphore()

    def greet(index):
        pl.semaphore_signal(
            barrier, inc=1, device_id=device(index), device_id_type=pl.DeviceIdType.MESH
        )

    for mask in greeted:
        greet(toggled(me, mask))
    if panels > 2:
        pl.when(middle)(lambda: greet(side_safe))

    def remote(source, target, send, recv, index):
        return pltpu.make_async_remote_copy(
            src_ref=source,
            dst_ref=target,
            send_sem=send,
            recv_sem=recv,
            device_id=device(index),
            device_id_type=pl.DeviceIdType.MESH,
        )

    scale = jnp.concatenate(
        [jnp.full((rank, 1), 1.0 / math.sqrt(leaf_size << level), f32) for level in range(levels)],
        axis=0,
    )
    top = local * rank

    def rows_of(level):
        return slice(level * rank, (level + 1) * rank)

    def first_half(x):
        return x[:, :rank]

    def second_half(x):
        return x[:, rank:]

    basis_copy.wait()
    coupling_copy.wait()
    basis = basis_ref[...].reshape(levels * rank, points)
    coupling = [coupling_ref[0, level] for level in range(levels)]
    bases = [basis[:, leaf * leaf_size : (leaf + 1) * leaf_size] for leaf in range(leaf_count)]
    grams = [nt(one, one) for one in bases]
    gram = sum(one[top:, top:] for one in grams)
    moved = [
        scale[top:] * triple(gram[:, rows_of(k)], coupling[local + k]) for k in range(depth)
    ]
    crossing = [moved[k][(k + 1) * rank :] for k in range(depth - 1)]
    cross_rows, cross_starts, cross_slots = spans(depth, rank, "cross")
    upper_rows, upper_starts, upper_slots = spans(depth, rank, "upper")
    for b in range(depth - 1):
        parts = [second_half(crossing[b])] + [
            first_half(crossing[j]) for j in range(b + 1, depth - 1)
        ]
        cross_sent[pl.ds(cross_starts[b], cross_rows[b])] = fold(jnp.concatenate(parts, axis=0))

    def spread(b, mask, source, target, rows, starts, slots, send, recv):
        place = slots[b] + (mask - (1 << b)) * rows[b]
        remote(
            source.at[pl.ds(starts[b], rows[b])],
            target.at[pl.ds(place, rows[b])],
            send.at[0],
            recv.at[0],
            toggled(me, mask),
        ).start()

    def spread_upper(b, mask):
        spread(
            b,
            mask,
            upper_sent,
            upper_received,
            upper_rows,
            upper_starts,
            upper_slots,
            upper_send,
            upper_recv,
        )

    extra = middle.astype(jnp.int32) if panels > 2 else 0
    pl.semaphore_wait(barrier, len(greeted) + extra)
    for b in range(depth - 1):
        for mask in range(1 << b, 2 << b):
            spread(
                b,
                mask,
                cross_sent,
                cross_received,
                cross_rows,
                cross_starts,
                cross_slots,
                cross_send,
                cross_recv,
            )
    train_copy.wait()
    mate_coords = remote(train_ref, coord_window.at[0], coord_send.at[0], coord_recv.at[0], mate)
    side_coords = remote(
        train_ref, coord_window.at[1], coord_send.at[1], coord_recv.at[1], side_safe
    )
    mate_coords.start()
    pl.when(has_side)(side_coords.start)

    def transfer(gram, level):
        below = (level + 1) * rank
        return scale[below:] * triple(gram[below:, rows_of(level)], coupling[level])

    local_sides = []
    for level in range(local):
        width = 1 << level
        parts = [
            transfer(sum(grams[c * width + i] for i in range(width)), level)
            for c in range(leaf_count // width)
        ]
        local_sides.append(
            [first_half(parts[c]) + second_half(parts[c ^ 1]) for c in range(len(parts))]
        )

    order_copy.wait()
    targets_copy.wait()
    inverse_copy.wait()
    near_copy.wait()
    test_copy.wait()
    stacked = jnp.concatenate(
        [targets_ref[:, h * CHUNK : (h + 1) * CHUNK] for h in range(points // CHUNK)], axis=0
    )
    order = order_ref[...]
    low, high = lax.rem(order, CHUNK), lax.div(order, CHUNK)
    solved, coefs = [], []
    for leaf in range(leaf_count):
        span = slice(leaf * leaf_size, (leaf + 1) * leaf_size)
        places = lax.broadcasted_iota(jnp.int32, (CHUNK, leaf_size), 0)
        chosen = jnp.where(places == low[:, span], 1.0, 0.0).astype(bf16)
        picked = nn(stacked, chosen)
        taken = jnp.zeros((columns, leaf_size), f32)
        for h in range(points // CHUNK):
            taken = jnp.where(
                high[:, span] == h, picked[h * columns : (h + 1) * columns], taken
            )
        state = nt(taken.astype(bf16), inverse_ref[leaf])
        state_high, state_low = halves(state)
        coefs.append((nt(bases[leaf], state_high) + nt(bases[leaf], state_low)) * scale)
        solved.append(state)

    mixes = [[] for _ in range(leaf_count)]
    for level in range(local):
        sides = local_sides[level]
        heads = [one[:rank] for one in coefs]
        for leaf in range(leaf_count):
            c = leaf >> level
            if leaf == c << level:
                mixed = triple(
                    coupling[level], jnp.concatenate([heads[c], heads[c ^ 1]], axis=0)
                )
            mixes[leaf].append(mixed)
        coefs = [
            coefs[2 * p][rank:]
            + coefs[2 * p + 1][rank:]
            - triple(sides[2 * p], heads[2 * p])
            - triple(sides[2 * p + 1], heads[2 * p + 1])
            for p in range(len(coefs) // 2)
        ]
    own = coefs[0]

    gain = 3.0 / (length_scale * length_scale) * math.log2(math.e) ** 2

    def norm(pos):
        return gain * (pos[0:1] * pos[0:1] + pos[1:2] * pos[1:2] + pos[2:3] * pos[2:3])

    def train_side(pos):
        ones = jnp.ones((3, points), f32)
        zero = jnp.zeros((1, points), f32)
        parts = thirds(-2.0 * gain * pos) + thirds(norm(pos)) + [ones, zero + GUARD]
        return jnp.concatenate(parts, axis=0).astype(bf16)

    def put_features(panel, pos):
        made = train_side(pos.astype(f32))
        for leaf in range(leaf_count):
            features[panel * leaf_count + leaf] = made[:, leaf * leaf_size : (leaf + 1) * leaf_size]

    test_pos = test_ref[...].astype(f32)
    ones = jnp.ones((3, tests), f32)
    zero = jnp.zeros((1, tests), f32)
    test_features[...] = jnp.concatenate(
        [test_pos, test_pos, test_pos, ones] + thirds(norm(test_pos)) + [zero + 1.0], axis=0
    ).astype(bf16)
    put_features(0, train_ref[...])
    for leaf in range(leaf_count):
        mix_high, mix_low = halves(jnp.concatenate(mixes[leaf], axis=0))
        solved[leaf] = (
            solved[leaf] - tn(mix_high, bases[leaf][:top]) - tn(mix_low, bases[leaf][:top])
        )

    remote(cross_received, cross_received, cross_send.at[0], cross_recv.at[0], mate).wait()
    summed = []
    for b in range(depth - 1):
        flat = unfold(
            sum(
                cross_received[pl.ds(cross_slots[b] + i * cross_rows[b], cross_rows[b])]
                for i in range(1 << b)
            )
        )
        pieces, place = {}, 0
        for j in range(b, depth - 1):
            size = (depth - 1 - j) * rank
            pieces[j] = flat[place : place + size]
            place += size
        summed.append(pieces)
    rest, flows = own, []
    for j in range(depth):
        flows.append(rest[:rank])
        if j < depth - 1:
            side_sum = first_half(crossing[j]) + sum(summed[b][j] for b in range(j + 1))
            rest = rest[rank:] - triple(side_sum, flows[j])
    for k in range(depth):
        sent[k] = pair(flows[k]).astype(bf16)
    unit_starts, units = [0], 0
    for mask in range(1, panels):
        unit_starts.append(units)
        units += depth - (mask.bit_length() - 1)
    for mask in reversed(range(1, panels)):
        b = mask.bit_length() - 1
        remote(
            sent.at[pl.ds(b, depth - b)],
            received.at[pl.ds(unit_starts[mask], depth - b)],
            round_send.at[0],
            round_recv.at[0],
            toggled(me, mask),
        ).start()
    for b in range(depth):
        parts = [moved[j][rows_of(b)] for j in range(b, depth)]
        upper_sent[pl.ds(upper_starts[b], upper_rows[b])] = pair(
            jnp.concatenate(parts, axis=0)
        ).astype(bf16)

    def within(place):
        return jnp.clip(place + 1, 0, 1) * jnp.clip(leaf_count - place, 0, 1)

    def window_leaf(slot):
        leaf_id = near_ref[0, slot]
        in_own = leaf_id - me * leaf_count
        in_mate = leaf_id - mate * leaf_count
        in_side = jnp.clip(leaf_id - side * leaf_count, 0, leaf_count - 1)
        is_own, is_mate = within(in_own), within(in_mate)
        return (
            is_own * in_own
            + is_mate * (leaf_count + in_mate)
            + (1 - is_own - is_mate) * (2 * leaf_count + in_side)
        )

    tiles = tests // TILE

    def near_block(slot, carry):
        squared = tn(features[window_leaf(slot)], test_features[...])
        scaled = squared * lax.rsqrt(squared)
        value = (scaled + 1.0 / math.log(2.0)) * jnp.exp2(
            math.log2(variance * math.log(2.0)) - scaled
        )
        rows = pl.ds(pl.multiple_of(slot * leaf_size, leaf_size), leaf_size)
        blocks[rows] = value.astype(bf16)
        return carry

    early = near * EARLY // 8
    middle_slot = near * MIDDLE // 8

    mate_coords.wait()
    put_features(1, coord_window[0])
    pl.when(has_side)(side_coords.wait)
    put_features(2, coord_window[1])
    lax.fori_loop(0, early // 2, near_block, 0, unroll=2)
    for b in range(depth):
        for mask in range(1 << b, 2 << b):
            spread_upper(b, mask)
    lax.fori_loop(early // 2, early, near_block, 0, unroll=2)

    remote(received, received, round_send.at[0], round_recv.at[0], mate).wait()
    mines, others, mixed_far = [], [], []

    def gathered(masks, k):
        return unpair(
            sum(
                received[unit_starts[mask] + k - (mask.bit_length() - 1)].astype(f32)
                for mask in masks
            )
        )

    for k in range(depth):
        mine = flows[k]
        if k:
            mine = mine + gathered(range(1, 1 << k), k)
        other = gathered(range(1 << k, 2 << k), k)
        mines.append(mine)
        others.append(other)
        mixed_far.append(triple(coupling[local + k], jnp.concatenate([mine, other], axis=0)))

    far_mix_high, far_mix_low = halves(jnp.concatenate(mixed_far, axis=0))
    for leaf in range(leaf_count):
        upper_basis = bases[leaf][top:]
        state = solved[leaf] - tn(far_mix_high, upper_basis) - tn(far_mix_low, upper_basis)
        weight_window[leaf] = state.astype(bf16)
        copy = remote(
            weight_window.at[leaf],
            weight_window.at[2 * leaf_count + leaf],
            side_send.at[0],
            side_recv.at[0],
            side_safe,
        )
        pl.when(has_side)(copy.start)

    def panel_of(index):
        return weight_window.at[pl.ds(index * leaf_count, leaf_count)]

    mate_weights = remote(panel_of(0), panel_of(1), pair_send.at[0], pair_recv.at[0], mate)
    mate_weights.start()
    side_weights = remote(panel_of(0), panel_of(2), side_send.at[0], side_recv.at[0], side_safe)

    lax.fori_loop(early, middle_slot, near_block, 0, unroll=2)
    remote(upper_received, upper_received, upper_send.at[0], upper_recv.at[0], mate).wait()
    far_rows = []
    for b in range(depth):
        flat = unpair(
            sum(
                upper_received[pl.ds(upper_slots[b] + i * upper_rows[b], upper_rows[b])].astype(f32)
                for i in range(1 << b)
            )
        )
        row = others[b]
        for j in range(b, depth):
            joined = [others[j], mines[j]] if j == b else [mines[j], others[j]]
            row = row - triple(flat[rows_of(j - b)], jnp.concatenate(joined, axis=0))
        far_rows.append(row)
    far_high, far_low = halves(jnp.concatenate(far_rows, axis=0))
    test_basis_copy.wait()
    test_basis = test_basis_ref[...].reshape(depth * rank, tests)
    far_sum[...] = tn(far_high, test_basis) + tn(far_low, test_basis)
    lax.fori_loop(middle_slot, near, near_block, 0, unroll=2)

    mate_weights.wait()
    pl.when(has_side)(side_weights.wait)
    held = jnp.concatenate([weight_window[window_leaf(slot)] for slot in range(near)], axis=1)
    for tile in range(tiles):
        lanes = slice(tile * TILE, (tile + 1) * TILE)
        near_sum = nn(held, blocks[:, lanes])
        out_ref[:, lanes] = (
            near_sum * (1.0 / math.sqrt(near * leaf_size)) + far_sum[:, lanes]
        ).astype(bf16)
        pltpu.make_async_copy(
            out_ref.at[:, lanes], out_hbm.at[:, lanes], out_sems.at[0]
        ).start()
    pltpu.make_async_copy(out_ref, out_hbm, out_sems.at[0]).wait()


def shards(
    panels,
    sub_size,
    targets,
    tree_order,
    leaf_inverse,
    cluster_basis,
    coupling,
    train_coords,
    test_coords,
    test_basis,
    near_leaves,
):
    columns, points = targets.shape
    leaf_count, leaf_size = leaf_inverse.shape[0], leaf_inverse.shape[1]
    levels, rank = cluster_basis.shape[0], cluster_basis.shape[1]
    near = near_leaves.shape[1]
    tests = test_coords.shape[1]
    depth = levels - (leaf_count.bit_length() - 1)
    cross_starts, cross_slots = spans(depth, rank, "cross")[1:]
    upper_starts, upper_slots = spans(depth, rank, "upper")[1:]
    units = sum((depth - b) << b for b in range(depth))
    anywhere = pl.BlockSpec(memory_space=pl.ANY)
    sems = pltpu.SemaphoreType.DMA
    operands = (
        tree_order,
        targets,
        leaf_inverse,
        cluster_basis,
        coupling,
        train_coords,
        test_coords,
        test_basis,
    )
    return pl.pallas_call(
        functools.partial(kernel, panels, sub_size),
        out_shape=jax.ShapeDtypeStruct((columns, tests), bf16),
        in_specs=[anywhere] * 9,
        out_specs=anywhere,
        scratch_shapes=[pltpu.VMEM(one.shape, one.dtype) for one in operands]
        + [
            pltpu.SMEM(near_leaves.shape, near_leaves.dtype),
            pltpu.VMEM((columns, tests), bf16),
            pltpu.VMEM((cross_starts[-1], 4 * rank), f32),
            pltpu.VMEM((cross_slots[-1], 4 * rank), f32),
            pltpu.VMEM((upper_starts[-1], 4 * rank), bf16),
            pltpu.VMEM((upper_slots[-1], 4 * rank), bf16),
            pltpu.VMEM((depth, rank // 2, 2 * columns), bf16),
            pltpu.VMEM((units, rank // 2, 2 * columns), bf16),
            pltpu.VMEM((2, 3, points), bf16),
            pltpu.VMEM((3 * leaf_count, FEATS, leaf_size), bf16),
            pltpu.VMEM((FEATS, tests), bf16),
            pltpu.VMEM((near * leaf_size, tests), bf16),
            pltpu.VMEM((3 * leaf_count, columns, leaf_size), bf16),
            pltpu.VMEM((columns, tests), f32),
            sems((9,)),
            sems((1,)),
            sems((1,)),
            sems((1,)),
            sems((1,)),
            sems((1,)),
            sems((1,)),
            sems((1,)),
            sems((2,)),
            sems((2,)),
            sems((1,)),
            sems((1,)),
            sems((1,)),
            sems((1,)),
        ],
        compiler_params=pltpu.CompilerParams(
            collective_id=0, has_side_effects=True, vmem_limit_bytes=60 * 1024 * 1024
        ),
    )(*operands, near_leaves)


def solution(mesh):
    return jax.shard_map(
        functools.partial(shards, mesh.shape["leaf"] * mesh.shape["sub"], mesh.shape["sub"]),
        mesh=mesh,
        in_specs=(
            P(None, ("grp", "leaf", "sub")),
            P(("grp", "leaf", "sub"), None),
            P(("grp", "leaf", "sub"), None, None),
            P(None, None, ("grp", "leaf", "sub")),
            P(("grp", "leaf", "sub"), None, None, None),
            P(None, ("grp", "leaf", "sub")),
            P(None, ("grp", "leaf", "sub")),
            P(None, None, ("grp", "leaf", "sub")),
            P(("grp", "leaf", "sub"), None),
        ),
        out_specs=P(None, ("grp", "leaf", "sub")),
        check_vma=False,
    )
```

```python
import functools
import math

import jax
import jax.numpy as jnp
from jax import lax
from jax.experimental import pallas as pl
from jax.experimental.pallas import tpu as pltpu
from jax.sharding import PartitionSpec as P

variance = 2.0
length_scale = 0.5
f32 = jnp.float32
bf16 = jnp.bfloat16
CHUNK = 256
TILE = 1024
FEATS = 16
EARLY = 4
MIDDLE = 6
GUARD = 2.0**-12


def nt(a, b):
    return lax.dot_general(a, b, (((1,), (1,)), ((), ())), preferred_element_type=f32)


def nn(a, b):
    return jnp.dot(a, b, preferred_element_type=f32)


def tn(a, b):
    return lax.dot_general(a, b, (((0,), (0,)), ((), ())), preferred_element_type=f32)


def halves(x):
    high = x.astype(bf16)
    return high, (x - high.astype(f32)).astype(bf16)


def thirds(x):
    first = x.astype(bf16).astype(f32)
    second = (x - first).astype(bf16).astype(f32)
    return [first, second, (x - first - second).astype(bf16).astype(f32)]


def toggled(index, mask):
    bit = 1
    while bit <= mask:
        if mask & bit:
            index = index + bit - 2 * bit * lax.rem(lax.div(index, bit), 2)
        bit *= 2
    return index


def triple(a, b):
    ah, al = halves(a)
    bh, bl = halves(b)
    return nn(ah, bh) + nn(ah, bl) + nn(al, bh)


def fold(x):
    rows = x.shape[0] // 4
    return jnp.concatenate([x[q * rows : (q + 1) * rows] for q in range(4)], axis=1)


def unfold(x):
    width = x.shape[1] // 4
    return jnp.concatenate([x[:, q * width : (q + 1) * width] for q in range(4)], axis=0)


def pair(x):
    rows = x.shape[0] // 2
    return jnp.concatenate([x[:rows], x[rows:]], axis=1)


def unpair(x):
    width = x.shape[1] // 2
    return jnp.concatenate([x[:, :width], x[:, width:]], axis=0)


def spans(depth, rank, parts):
    cross = [sum((depth - 1 - j) * rank for j in range(b, depth - 1)) // 4 for b in range(depth)]
    upper = [(depth - b) * rank // 2 for b in range(depth)]
    rows = cross if parts == "cross" else upper
    starts = [sum(rows[:b]) for b in range(depth + 1)]
    slots = [sum((1 << c) * rows[c] for c in range(b)) for b in range(depth + 1)]
    return rows, starts, slots


def kernel(
    panels,
    sub_size,
    order_hbm,
    targets_hbm,
    inverse_hbm,
    basis_hbm,
    coupling_hbm,
    train_hbm,
    test_hbm,
    test_basis_hbm,
    near_hbm,
    out_hbm,
    order_ref,
    targets_ref,
    inverse_ref,
    basis_ref,
    coupling_ref,
    train_ref,
    test_ref,
    test_basis_ref,
    near_ref,
    out_ref,
    cross_sent,
    cross_received,
    upper_sent,
    upper_received,
    sent,
    received,
    coord_window,
    features,
    test_features,
    blocks,
    weight_window,
    far_sum,
    load_sems,
    out_sems,
    cross_send,
    cross_recv,
    upper_send,
    upper_recv,
    round_send,
    round_recv,
    coord_send,
    coord_recv,
    pair_send,
    pair_recv,
    side_send,
    side_recv,
):
    columns, points = targets_ref.shape
    leaf_count, leaf_size = inverse_ref.shape[0], inverse_ref.shape[1]
    levels, rank = basis_ref.shape[0], basis_ref.shape[1]
    near = near_ref.shape[1]
    tests = test_ref.shape[1]
    local = leaf_count.bit_length() - 1
    depth = levels - local
    half = panels // 2
    me = lax.axis_index("leaf") * sub_size + lax.axis_index("sub")

    def load(index, source, target):
        copy = pltpu.make_async_copy(source, target, load_sems.at[index])
        copy.start()
        return copy

    basis_copy = load(0, basis_hbm, basis_ref)
    coupling_copy = load(1, coupling_hbm, coupling_ref)
    order_copy = load(2, order_hbm, order_ref)
    targets_copy = load(3, targets_hbm, targets_ref)
    inverse_copy = load(8, inverse_hbm, inverse_ref)
    train_copy = load(4, train_hbm, train_ref)
    test_copy = load(5, test_hbm, test_ref)
    near_copy = load(6, near_hbm, near_ref)
    test_basis_copy = load(7, test_basis_hbm, test_basis_ref)

    def device(index):
        return {"leaf": lax.div(index, sub_size), "sub": lax.rem(index, sub_size)}

    odd = lax.rem(me, 2)
    mate = me + 1 - 2 * odd
    side = me - 1 + 2 * odd
    has_side = (side >= 0) & (side < panels)
    side_safe = jnp.clip(side, 0, panels - 1)
    middle = (me == half - 1) | (me == half)
    greeted = list(range(1, half)) + [half]

    barrier = pltpu.get_barrier_semaphore()

    def greet(index):
        pl.semaphore_signal(
            barrier, inc=1, device_id=device(index), device_id_type=pl.DeviceIdType.MESH
        )

    for mask in greeted:
        greet(toggled(me, mask))
    if panels > 2:
        pl.when(middle)(lambda: greet(side_safe))

    def remote(source, target, send, recv, index):
        return pltpu.make_async_remote_copy(
            src_ref=source,
            dst_ref=target,
            send_sem=send,
            recv_sem=recv,
            device_id=device(index),
            device_id_type=pl.DeviceIdType.MESH,
        )

    scale = jnp.concatenate(
        [jnp.full((rank, 1), 1.0 / math.sqrt(leaf_size << level), f32) for level in range(levels)],
        axis=0,
    )
    top = local * rank

    def rows_of(level):
        return slice(level * rank, (level + 1) * rank)

    def first_half(x):
        return x[:, :rank]

    def second_half(x):
        return x[:, rank:]

    basis_copy.wait()
    coupling_copy.wait()
    basis = basis_ref[...].reshape(levels * rank, points)
    coupling = [coupling_ref[0, level] for level in range(levels)]
    bases = [basis[:, leaf * leaf_size : (leaf + 1) * leaf_size] for leaf in range(leaf_count)]
    grams = [nt(one, one) for one in bases]
    gram = sum(one[top:, top:] for one in grams)
    moved = [
        scale[top:] * triple(gram[:, rows_of(k)], coupling[local + k]) for k in range(depth)
    ]
    crossing = [moved[k][(k + 1) * rank :] for k in range(depth - 1)]
    cross_rows, cross_starts, cross_slots = spans(depth, rank, "cross")
    upper_rows, upper_starts, upper_slots = spans(depth, rank, "upper")
    for b in range(depth - 1):
        parts = [second_half(crossing[b])] + [
            first_half(crossing[j]) for j in range(b + 1, depth - 1)
        ]
        cross_sent[pl.ds(cross_starts[b], cross_rows[b])] = fold(jnp.concatenate(parts, axis=0))

    def spread(b, mask, source, target, rows, starts, slots, send, recv):
        place = slots[b] + (mask - (1 << b)) * rows[b]
        remote(
            source.at[pl.ds(starts[b], rows[b])],
            target.at[pl.ds(place, rows[b])],
            send.at[0],
            recv.at[0],
            toggled(me, mask),
        ).start()

    def spread_upper(b, mask):
        spread(
            b,
            mask,
            upper_sent,
            upper_received,
            upper_rows,
            upper_starts,
            upper_slots,
            upper_send,
            upper_recv,
        )

    extra = middle.astype(jnp.int32) if panels > 2 else 0
    pl.semaphore_wait(barrier, len(greeted) + extra)
    for b in range(depth - 1):
        for mask in range(1 << b, 2 << b):
            spread(
                b,
                mask,
                cross_sent,
                cross_received,
                cross_rows,
                cross_starts,
                cross_slots,
                cross_send,
                cross_recv,
            )
    train_copy.wait()
    mate_coords = remote(train_ref, coord_window.at[0], coord_send.at[0], coord_recv.at[0], mate)
    side_coords = remote(
        train_ref, coord_window.at[1], coord_send.at[1], coord_recv.at[1], side_safe
    )
    mate_coords.start()
    pl.when(has_side)(side_coords.start)

    def transfer(gram, level):
        below = (level + 1) * rank
        return scale[below:] * triple(gram[below:, rows_of(level)], coupling[level])

    local_sides = []
    for level in range(local):
        width = 1 << level
        parts = [
            transfer(sum(grams[c * width + i] for i in range(width)), level)
            for c in range(leaf_count // width)
        ]
        local_sides.append(
            [first_half(parts[c]) + second_half(parts[c ^ 1]) for c in range(len(parts))]
        )

    order_copy.wait()
    targets_copy.wait()
    inverse_copy.wait()
    near_copy.wait()
    test_copy.wait()
    stacked = jnp.concatenate(
        [targets_ref[:, h * CHUNK : (h + 1) * CHUNK] for h in range(points // CHUNK)], axis=0
    )
    order = order_ref[...]
    low, high = lax.rem(order, CHUNK), lax.div(order, CHUNK)
    solved, coefs = [], []
    for leaf in range(leaf_count):
        span = slice(leaf * leaf_size, (leaf + 1) * leaf_size)
        places = lax.broadcasted_iota(jnp.int32, (CHUNK, leaf_size), 0)
        chosen = jnp.where(places == low[:, span], 1.0, 0.0).astype(bf16)
        picked = nn(stacked, chosen)
        taken = jnp.zeros((columns, leaf_size), f32)
        for h in range(points // CHUNK):
            taken = jnp.where(
                high[:, span] == h, picked[h * columns : (h + 1) * columns], taken
            )
        state = nt(taken.astype(bf16), inverse_ref[leaf])
        state_high, state_low = halves(state)
        coefs.append((nt(bases[leaf], state_high) + nt(bases[leaf], state_low)) * scale)
        solved.append(state)

    mixes = [[] for _ in range(leaf_count)]
    for level in range(local):
        sides = local_sides[level]
        heads = [one[:rank] for one in coefs]
        for leaf in range(leaf_count):
            c = leaf >> level
            if leaf == c << level:
                mixed = triple(
                    coupling[level], jnp.concatenate([heads[c], heads[c ^ 1]], axis=0)
                )
            mixes[leaf].append(mixed)
        coefs = [
            coefs[2 * p][rank:]
            + coefs[2 * p + 1][rank:]
            - triple(sides[2 * p], heads[2 * p])
            - triple(sides[2 * p + 1], heads[2 * p + 1])
            for p in range(len(coefs) // 2)
        ]
    own = coefs[0]

    gain = 3.0 / (length_scale * length_scale) * math.log2(math.e) ** 2

    def norm(pos):
        return gain * (pos[0:1] * pos[0:1] + pos[1:2] * pos[1:2] + pos[2:3] * pos[2:3])

    def train_side(pos):
        ones = jnp.ones((3, points), f32)
        zero = jnp.zeros((1, points), f32)
        parts = thirds(-2.0 * gain * pos) + thirds(norm(pos)) + [ones, zero + GUARD]
        return jnp.concatenate(parts, axis=0).astype(bf16)

    def put_features(panel, pos):
        made = train_side(pos.astype(f32))
        for leaf in range(leaf_count):
            features[panel * leaf_count + leaf] = made[:, leaf * leaf_size : (leaf + 1) * leaf_size]

    test_pos = test_ref[...].astype(f32)
    ones = jnp.ones((3, tests), f32)
    zero = jnp.zeros((1, tests), f32)
    test_features[...] = jnp.concatenate(
        [test_pos, test_pos, test_pos, ones] + thirds(norm(test_pos)) + [zero + 1.0], axis=0
    ).astype(bf16)
    put_features(0, train_ref[...])
    for leaf in range(leaf_count):
        mix_high, mix_low = halves(jnp.concatenate(mixes[leaf], axis=0))
        solved[leaf] = (
            solved[leaf] - tn(mix_high, bases[leaf][:top]) - tn(mix_low, bases[leaf][:top])
        )

    remote(cross_received, cross_received, cross_send.at[0], cross_recv.at[0], mate).wait()
    summed = []
    for b in range(depth - 1):
        flat = unfold(
            sum(
                cross_received[pl.ds(cross_slots[b] + i * cross_rows[b], cross_rows[b])]
                for i in range(1 << b)
            )
        )
        pieces, place = {}, 0
        for j in range(b, depth - 1):
            size = (depth - 1 - j) * rank
            pieces[j] = flat[place : place + size]
            place += size
        summed.append(pieces)
    rest, flows = own, []
    for j in range(depth):
        flows.append(rest[:rank])
        if j < depth - 1:
            side_sum = first_half(crossing[j]) + sum(summed[b][j] for b in range(j + 1))
            rest = rest[rank:] - triple(side_sum, flows[j])
    for k in range(depth):
        sent[k] = pair(flows[k])
    unit_starts, units = [0], 0
    for mask in range(1, panels):
        unit_starts.append(units)
        units += depth - (mask.bit_length() - 1)
    for mask in reversed(range(1, panels)):
        b = mask.bit_length() - 1
        remote(
            sent.at[pl.ds(b, depth - b)],
            received.at[pl.ds(unit_starts[mask], depth - b)],
            round_send.at[0],
            round_recv.at[0],
            toggled(me, mask),
        ).start()
    for b in range(depth):
        parts = [moved[j][rows_of(b)] for j in range(b, depth)]
        upper_sent[pl.ds(upper_starts[b], upper_rows[b])] = pair(
            jnp.concatenate(parts, axis=0)
        ).astype(bf16)

    def within(place):
        return jnp.clip(place + 1, 0, 1) * jnp.clip(leaf_count - place, 0, 1)

    def window_leaf(slot):
        leaf_id = near_ref[0, slot]
        in_own = leaf_id - me * leaf_count
        in_mate = leaf_id - mate * leaf_count
        in_side = jnp.clip(leaf_id - side * leaf_count, 0, leaf_count - 1)
        is_own, is_mate = within(in_own), within(in_mate)
        return (
            is_own * in_own
            + is_mate * (leaf_count + in_mate)
            + (1 - is_own - is_mate) * (2 * leaf_count + in_side)
        )

    tiles = tests // TILE

    def near_block(slot, carry):
        squared = tn(features[window_leaf(slot)], test_features[...])
        scaled = squared * lax.rsqrt(squared)
        value = (scaled + 1.0 / math.log(2.0)) * jnp.exp2(
            math.log2(variance * math.log(2.0)) - scaled
        )
        rows = pl.ds(pl.multiple_of(slot * leaf_size, leaf_size), leaf_size)
        blocks[rows] = value.astype(bf16)
        return carry

    early = near * EARLY // 8
    middle_slot = near * MIDDLE // 8

    mate_coords.wait()
    put_features(1, coord_window[0])
    pl.when(has_side)(side_coords.wait)
    put_features(2, coord_window[1])
    lax.fori_loop(0, early // 2, near_block, 0, unroll=2)
    for b in range(depth):
        for mask in range(1 << b, 2 << b):
            spread_upper(b, mask)
    lax.fori_loop(early // 2, early, near_block, 0, unroll=2)

    remote(received, received, round_send.at[0], round_recv.at[0], mate).wait()
    mines, others, mixed_far = [], [], []

    def gathered(masks, k):
        return unpair(
            sum(
                received[unit_starts[mask] + k - (mask.bit_length() - 1)]
                for mask in masks
            )
        )

    for k in range(depth):
        mine = flows[k]
        if k:
            mine = mine + gathered(range(1, 1 << k), k)
        other = gathered(range(1 << k, 2 << k), k)
        mines.append(mine)
        others.append(other)
        mixed_far.append(triple(coupling[local + k], jnp.concatenate([mine, other], axis=0)))

    far_mix_high, far_mix_low = halves(jnp.concatenate(mixed_far, axis=0))
    for leaf in range(leaf_count):
        upper_basis = bases[leaf][top:]
        state = solved[leaf] - tn(far_mix_high, upper_basis) - tn(far_mix_low, upper_basis)
        weight_window[leaf] = state.astype(bf16)
        copy = remote(
            weight_window.at[leaf],
            weight_window.at[2 * leaf_count + leaf],
            side_send.at[0],
            side_recv.at[0],
            side_safe,
        )
        pl.when(has_side)(copy.start)

    def panel_of(index):
        return weight_window.at[pl.ds(index * leaf_count, leaf_count)]

    mate_weights = remote(panel_of(0), panel_of(1), pair_send.at[0], pair_recv.at[0], mate)
    mate_weights.start()
    side_weights = remote(panel_of(0), panel_of(2), side_send.at[0], side_recv.at[0], side_safe)

    lax.fori_loop(early, middle_slot, near_block, 0, unroll=2)
    remote(upper_received, upper_received, upper_send.at[0], upper_recv.at[0], mate).wait()
    far_rows = []
    for b in range(depth):
        flat = unpair(
            sum(
                upper_received[pl.ds(upper_slots[b] + i * upper_rows[b], upper_rows[b])].astype(f32)
                for i in range(1 << b)
            )
        )
        row = others[b]
        for j in range(b, depth):
            joined = [others[j], mines[j]] if j == b else [mines[j], others[j]]
            row = row - triple(flat[rows_of(j - b)], jnp.concatenate(joined, axis=0))
        far_rows.append(row)
    far_high, far_low = halves(jnp.concatenate(far_rows, axis=0))
    test_basis_copy.wait()
    test_basis = test_basis_ref[...].reshape(depth * rank, tests)
    far_sum[...] = tn(far_high, test_basis) + tn(far_low, test_basis)
    lax.fori_loop(middle_slot, near, near_block, 0, unroll=2)

    mate_weights.wait()
    pl.when(has_side)(side_weights.wait)
    held = jnp.concatenate([weight_window[window_leaf(slot)] for slot in range(near)], axis=1)
    for tile in range(tiles):
        lanes = slice(tile * TILE, (tile + 1) * TILE)
        near_sum = nn(held, blocks[:, lanes])
        out_ref[:, lanes] = (
            near_sum * (1.0 / math.sqrt(near * leaf_size)) + far_sum[:, lanes]
        ).astype(bf16)
        pltpu.make_async_copy(
            out_ref.at[:, lanes], out_hbm.at[:, lanes], out_sems.at[0]
        ).start()
    pltpu.make_async_copy(out_ref, out_hbm, out_sems.at[0]).wait()


def shards(
    panels,
    sub_size,
    targets,
    tree_order,
    leaf_inverse,
    cluster_basis,
    coupling,
    train_coords,
    test_coords,
    test_basis,
    near_leaves,
):
    columns, points = targets.shape
    leaf_count, leaf_size = leaf_inverse.shape[0], leaf_inverse.shape[1]
    levels, rank = cluster_basis.shape[0], cluster_basis.shape[1]
    near = near_leaves.shape[1]
    tests = test_coords.shape[1]
    depth = levels - (leaf_count.bit_length() - 1)
    cross_starts, cross_slots = spans(depth, rank, "cross")[1:]
    upper_starts, upper_slots = spans(depth, rank, "upper")[1:]
    units = sum((depth - b) << b for b in range(depth))
    anywhere = pl.BlockSpec(memory_space=pl.ANY)
    sems = pltpu.SemaphoreType.DMA
    operands = (
        tree_order,
        targets,
        leaf_inverse,
        cluster_basis,
        coupling,
        train_coords,
        test_coords,
        test_basis,
    )
    return pl.pallas_call(
        functools.partial(kernel, panels, sub_size),
        out_shape=jax.ShapeDtypeStruct((columns, tests), bf16),
        in_specs=[anywhere] * 9,
        out_specs=anywhere,
        scratch_shapes=[pltpu.VMEM(one.shape, one.dtype) for one in operands]
        + [
            pltpu.SMEM(near_leaves.shape, near_leaves.dtype),
            pltpu.VMEM((columns, tests), bf16),
            pltpu.VMEM((cross_starts[-1], 4 * rank), f32),
            pltpu.VMEM((cross_slots[-1], 4 * rank), f32),
            pltpu.VMEM((upper_starts[-1], 4 * rank), bf16),
            pltpu.VMEM((upper_slots[-1], 4 * rank), bf16),
            pltpu.VMEM((depth, rank // 2, 2 * columns), f32),
            pltpu.VMEM((units, rank // 2, 2 * columns), f32),
            pltpu.VMEM((2, 3, points), bf16),
            pltpu.VMEM((3 * leaf_count, FEATS, leaf_size), bf16),
            pltpu.VMEM((FEATS, tests), bf16),
            pltpu.VMEM((near * leaf_size, tests), bf16),
            pltpu.VMEM((3 * leaf_count, columns, leaf_size), bf16),
            pltpu.VMEM((columns, tests), f32),
            sems((9,)),
            sems((1,)),
            sems((1,)),
            sems((1,)),
            sems((1,)),
            sems((1,)),
            sems((1,)),
            sems((1,)),
            sems((2,)),
            sems((2,)),
            sems((1,)),
            sems((1,)),
            sems((1,)),
            sems((1,)),
        ],
        compiler_params=pltpu.CompilerParams(
            collective_id=0, has_side_effects=True, vmem_limit_bytes=60 * 1024 * 1024
        ),
    )(*operands, near_leaves)


def solution(mesh):
    return jax.shard_map(
        functools.partial(shards, mesh.shape["leaf"] * mesh.shape["sub"], mesh.shape["sub"]),
        mesh=mesh,
        in_specs=(
            P(None, ("grp", "leaf", "sub")),
            P(("grp", "leaf", "sub"), None),
            P(("grp", "leaf", "sub"), None, None),
            P(None, None, ("grp", "leaf", "sub")),
            P(("grp", "leaf", "sub"), None, None, None),
            P(None, ("grp", "leaf", "sub")),
            P(None, ("grp", "leaf", "sub")),
            P(None, None, ("grp", "leaf", "sub")),
            P(("grp", "leaf", "sub"), None),
        ),
        out_specs=P(None, ("grp", "leaf", "sub")),
        check_vma=False,
    )
```
